32 devices in a mesh: dp: 1 (over z), tp: 32 (over y, x, core).
Axes of the slice: x: 4, y: 4, z: 1, core: 2. Of those that a mesh axis runs over, the one named last changes fastest.
The devices are a block of a 4x4x8 slice.
Arguments:
- y_one: float32 [96, 32, 2048], P('dp')
- y_two: float32 [96, 32, 2048], P('dp')
- dy_one: float32 [96, 32, 2048], P('dp')
- dy_two: float32 [96, 32, 2048], P('dp')
- seq_lens: int32 [96], P('dp')
- w_query: bfloat16 [1, 2048, 32, 64], P(None, None, 'tp')
- w_key: bfloat16 [1, 2048, 32, 64], P(None, None, 'tp')
- w_value: bfloat16 [1, 2048, 32, 64], P(None, None, 'tp')
- w_out: bfloat16 [1, 32, 64, 2048], P(None, 'tp')
- w_up: bfloat16 [1, 2048, 8192], P(None, None, 'tp')
- w_down: bfloat16 [1, 8192, 2048], P(None, 'tp')
Outputs:
- output 1: float32 [96, 32, 2048], P('dp')
- output 2: float32 [96, 32, 2048], P('dp')
- output 3: float32 [96, 32, 2048], P('dp')
- output 4: float32 [96, 32, 2048], P('dp')
- output 5: float32 [1, 2048, 32, 64], P('dp', None, 'tp')
- output 6: float32 [1, 2048, 32, 64], P('dp', None, 'tp')
- output 7: float32 [1, 2048, 32, 64], P('dp', None, 'tp')
- output 8: float32 [1, 32, 64, 2048], P('dp', 'tp')
- output 9: float32 [1, 2048, 8192], P('dp', None, 'tp')
- output 10: float32 [1, 8192, 2048], P('dp', 'tp')
All inputs are finite; a program needn't handle non-finite values.
Results may differ from the reference program's by a relative error of at most 0.00909588.
Values are sent between devices in bfloat16 or wider.
A program may use at most 768 MiB of HBM per device.

```python
import functools
import jax
import jax.numpy as jnp
from jax import lax

D = 2048
HEADS = 32
KV_HEADS = 8
HEAD = 64
FF = 8192
LAYERS = 1
SEQS = 3
SEQ = 32
TP = 32
KV_SLOTS = max(KV_HEADS, TP)
REPEAT = KV_SLOTS // KV_HEADS
GROUP = HEADS // KV_SLOTS
BATCH = SEQS * TP
TOKENS = BATCH * SEQ
EPS = 1e-5
SCORE_SCALE = HEAD ** -0.5
OUT_GAIN = 0.5 * (SEQ / 64) ** 0.25


def normal_weights(rng_key, arr_shape, scale_std):
    return (jax.random.normal(rng_key, arr_shape, jnp.float32) * scale_std).astype(jnp.bfloat16)


def draw_lengths(rng_key):
    len_key, top_key, low_key = jax.random.split(rng_key, 3)
    seq_lens = jax.random.randint(len_key, (BATCH,), SEQ // 4, SEQ + 1)
    top_idx = jax.random.randint(top_key, (), 0, BATCH)
    low_idx = (top_idx + jax.random.randint(low_key, (), 1, BATCH)) % BATCH
    positions = jnp.arange(BATCH)
    seq_lens = jnp.where(positions == top_idx, SEQ, seq_lens)
    seq_lens = jnp.where(positions == low_idx, SEQ // 4, seq_lens)
    return seq_lens.astype(jnp.int32)


def setup_inputs(seed: int = 0, part: int = 0) -> dict:
    weight_keys = jax.random.split(jax.random.key(seed), 6)
    part_keys = jax.random.split(jax.random.fold_in(jax.random.key(seed + 1), part), 5)
    act_shape = (BATCH, SEQ, D)
    key_heads = normal_weights(weight_keys[1], (LAYERS, D, KV_HEADS, HEAD), D ** -0.5)
    value_heads = normal_weights(weight_keys[2], (LAYERS, D, KV_HEADS, HEAD), D ** -0.5)
    return {
        'y_one': jax.random.normal(part_keys[0], act_shape, jnp.float32),
        'y_two': jax.random.normal(part_keys[1], act_shape, jnp.float32),
        'dy_one': jax.random.normal(part_keys[2], act_shape, jnp.float32),
        'dy_two': jax.random.normal(part_keys[3], act_shape, jnp.float32),
        'seq_lens': draw_lengths(part_keys[4]),
        'w_query': normal_weights(weight_keys[0], (LAYERS, D, HEADS, HEAD), 2.0 * D ** -0.5),
        'w_key': jnp.repeat(key_heads, REPEAT, axis=2),
        'w_value': jnp.repeat(value_heads, REPEAT, axis=2),
        'w_out': normal_weights(weight_keys[3], (LAYERS, HEADS, HEAD, D), OUT_GAIN * (HEADS * HEAD) ** -0.5),
        'w_up': normal_weights(weight_keys[4], (LAYERS, D, FF), D ** -0.5),
        'w_down': normal_weights(weight_keys[5], (LAYERS, FF, D), 0.6 * FF ** -0.5),
    }


def rms_norm(x_val):
    inv_rms = lax.rsqrt(jnp.mean(x_val * x_val, axis=-1, keepdims=True) + EPS)
    return x_val * inv_rms, inv_rms


def rms_back(normed, inv_rms, grad_norm):
    return inv_rms * (grad_norm - normed * jnp.mean(grad_norm * normed, axis=-1, keepdims=True))


def attend_seq(operands):
    q_seq, k_seq, v_seq, dout_seq, seq_len = operands
    q_grp = q_seq.reshape(SEQ, KV_SLOTS, GROUP, HEAD).astype(jnp.float32)
    k_full = k_seq.astype(jnp.float32)
    v_full = v_seq.astype(jnp.float32)
    dout_grp = dout_seq.reshape(SEQ, KV_SLOTS, GROUP, HEAD).astype(jnp.float32)
    row_pos = jnp.arange(SEQ)[:, None]
    col_pos = jnp.arange(SEQ)[None, :]
    visible = (col_pos <= row_pos) & (col_pos < seq_len)
    scores = jnp.einsum('igre,jge->grij', q_grp, k_full) * SCORE_SCALE
    scores = jnp.where(visible, scores, -1e30)
    attn_probs = jax.nn.softmax(scores, axis=-1)
    probs_b = attn_probs.astype(jnp.bfloat16).astype(jnp.float32)
    attn_out = jnp.einsum('grij,jge->igre', probs_b, v_full).astype(jnp.bfloat16)
    d_value = jnp.einsum('grij,igre->jge', probs_b, dout_grp).astype(jnp.bfloat16)
    d_probs = jnp.einsum('igre,jge->grij', dout_grp, v_full)
    d_scores = attn_probs * (d_probs - jnp.sum(d_probs * attn_probs, axis=-1, keepdims=True)) * SCORE_SCALE
    d_scores = d_scores.astype(jnp.bfloat16).astype(jnp.float32)
    d_query = jnp.einsum('grij,jge->igre', d_scores, k_full).astype(jnp.bfloat16)
    d_key = jnp.einsum('grij,igre->jge', d_scores, q_grp).astype(jnp.bfloat16)
    return attn_out.reshape(SEQ, HEADS, HEAD), d_query.reshape(SEQ, HEADS, HEAD), d_key, d_value


def layer_back(seq_lens, carry, layer_w):
    y_one, y_two, dy_one, dy_two = carry
    w_query, w_key, w_value, w_out, w_up, w_down = layer_w
    norm_g, inv_g = rms_norm(y_one.reshape(TOKENS, D))
    norm_g_b = norm_g.astype(jnp.bfloat16)
    pre_act = jnp.dot(norm_g_b, w_up, preferred_element_type=jnp.float32)
    act_val, gelu_back = jax.vjp(jax.nn.gelu, pre_act)
    act_b = act_val.astype(jnp.bfloat16)
    g_branch = jnp.dot(act_b, w_down, preferred_element_type=jnp.float32)
    x_two = y_two - g_branch.reshape(BATCH, SEQ, D)
    dy2_b = dy_two.reshape(TOKENS, D).astype(jnp.bfloat16)
    d_act = jnp.dot(dy2_b, w_down.T, preferred_element_type=jnp.float32)
    d_pre = gelu_back(d_act)[0].astype(jnp.bfloat16)
    dw_down = jnp.dot(act_b.T, dy2_b, preferred_element_type=jnp.float32)
    dw_up = jnp.dot(norm_g_b.T, d_pre, preferred_element_type=jnp.float32)
    grad_norm_g = jnp.dot(d_pre, w_up.T, preferred_element_type=jnp.float32)
    dy_one = dy_one + rms_back(norm_g, inv_g, grad_norm_g).reshape(BATCH, SEQ, D)

    norm_f, inv_f = rms_norm(x_two.reshape(TOKENS, D))
    norm_f_b = norm_f.astype(jnp.bfloat16)
    wq_flat = w_query.reshape(D, HEADS * HEAD)
    wk_flat = w_key.reshape(D, KV_SLOTS * HEAD)
    wv_flat = w_value.reshape(D, KV_SLOTS * HEAD)
    wo_flat = w_out.reshape(HEADS * HEAD, D)
    q_all = jnp.dot(norm_f_b, wq_flat, preferred_element_type=jnp.float32).astype(jnp.bfloat16).reshape(BATCH, SEQ, HEADS, HEAD)
    k_all = jnp.dot(norm_f_b, wk_flat, preferred_element_type=jnp.float32).astype(jnp.bfloat16).reshape(BATCH, SEQ, KV_SLOTS, HEAD)
    v_all = jnp.dot(norm_f_b, wv_flat, preferred_element_type=jnp.float32).astype(jnp.bfloat16).reshape(BATCH, SEQ, KV_SLOTS, HEAD)
    dy1_b = dy_one.reshape(TOKENS, D).astype(jnp.bfloat16)
    d_attn = jnp.dot(dy1_b, wo_flat.T, preferred_element_type=jnp.float32).astype(jnp.bfloat16).reshape(BATCH, SEQ, HEADS, HEAD)
    attn_out, d_query, d_key, d_value = lax.map(attend_seq, (q_all, k_all, v_all, d_attn, seq_lens))
    out_flat = attn_out.reshape(TOKENS, HEADS * HEAD)
    f_branch = jnp.dot(out_flat, wo_flat, preferred_element_type=jnp.float32)
    x_one = y_one - f_branch.reshape(BATCH, SEQ, D)
    dw_out = jnp.dot(out_flat.T, dy1_b, preferred_element_type=jnp.float32).reshape(HEADS, HEAD, D)
    dq_flat = d_query.reshape(TOKENS, HEADS * HEAD)
    dk_flat = d_key.reshape(TOKENS, KV_SLOTS * HEAD)
    dv_flat = d_value.reshape(TOKENS, KV_SLOTS * HEAD)
    dw_query = jnp.dot(norm_f_b.T, dq_flat, preferred_element_type=jnp.float32).reshape(D, HEADS, HEAD)
    dw_key = jnp.dot(norm_f_b.T, dk_flat, preferred_element_type=jnp.float32).reshape(D, KV_SLOTS, HEAD)
    dw_value = jnp.dot(norm_f_b.T, dv_flat, preferred_element_type=jnp.float32).reshape(D, KV_SLOTS, HEAD)
    grad_norm_f = (jnp.dot(dq_flat, wq_flat.T, preferred_element_type=jnp.float32)
                   + jnp.dot(dk_flat, wk_flat.T, preferred_element_type=jnp.float32)
                   + jnp.dot(dv_flat, wv_flat.T, preferred_element_type=jnp.float32))
    dx_two = dy_two + rms_back(norm_f, inv_f, grad_norm_f).reshape(BATCH, SEQ, D)
    return (x_one, x_two, dy_one, dx_two), (dw_query, dw_key, dw_value, dw_out, dw_up, dw_down)


def reference(y_one, y_two, dy_one, dy_two, seq_lens, w_query, w_key, w_value, w_out, w_up, w_down):
    end_state, layer_grads = lax.scan(functools.partial(layer_back, seq_lens), (y_one, y_two, dy_one, dy_two), (w_query, w_key, w_value, w_out, w_up, w_down), reverse=True)
    return (end_state[0], end_state[1], end_state[2], end_state[3], layer_grads[0], layer_grads[1], layer_grads[2], layer_grads[3], layer_grads[4], layer_grads[5])
```

```python
import functools

import jax
import jax.numpy as jnp
from jax import lax
from jax.experimental import pallas as pl
from jax.experimental.pallas import tpu as pltpu
from jax.sharding import PartitionSpec as P

F32 = jnp.float32
BF16 = jnp.bfloat16
EPS = 1e-5
MASK_VALUE = -1e30
GELU_COEF = 0.044715
GELU_SCALE = (2.0 / jnp.pi) ** 0.5
VMEM_LIMIT = 60 * 1024 * 1024
N_CHUNKS = 2
NN = (((1,), (0,)), ((), ()))
NT = (((1,), (1,)), ((), ()))
TN = (((0,), (0,)), ((), ()))


def dot(lhs, rhs, dims=NN):
    return lax.dot_general(lhs, rhs, dims, preferred_element_type=F32)


def rms_norm(x_val):
    inv_rms = lax.rsqrt(jnp.mean(x_val * x_val, axis=-1, keepdims=True) + EPS)
    return x_val * inv_rms, inv_rms


def rms_back(normed, inv_rms, grad_norm):
    return inv_rms * (grad_norm - normed * jnp.mean(grad_norm * normed, axis=-1, keepdims=True))


def gelu_and_slope(x_val):
    tanh_val = jnp.tanh(GELU_SCALE * (x_val + GELU_COEF * (x_val * x_val * x_val)))
    cdf = 0.5 * (1.0 + tanh_val)
    inner_slope = GELU_SCALE * (1.0 + 3.0 * GELU_COEF * (x_val * x_val))
    return x_val * cdf, cdf + x_val * (0.5 * (1.0 - tanh_val * tanh_val) * inner_slope)


def ffn_kernel(has_acc, *refs):
    y_ref, dy_ref, up_ref, down_ref = refs[:4]
    refs = refs[4:]
    if has_acc:
        up_acc, down_acc = refs[:2]
        refs = refs[2:]
    branch_ref, dnorm_ref, dup_ref, ddown_ref, up_t, down_t = refs

    @pl.when(pl.program_id(0) == 0)
    def _():
        up_t[...] = up_ref[...].T
        down_t[...] = down_ref[...].T
        dup_ref[...] = up_acc[...] if has_acc else jnp.zeros_like(dup_ref)
        ddown_ref[...] = down_acc[...] if has_acc else jnp.zeros_like(ddown_ref)

    norm_b = rms_norm(y_ref[...])[0].astype(BF16)
    dy_b = dy_ref[...].astype(BF16)
    act_val, slope = gelu_and_slope(dot(norm_b, up_ref[...]))
    act_b = act_val.astype(BF16)
    branch_ref[...] = dot(act_b, down_ref[...])
    d_pre = (slope * dot(dy_b, down_t[...])).astype(BF16)
    dnorm_ref[...] = dot(d_pre, up_t[...]).astype(BF16)
    ddown_ref[...] += dot(act_b, dy_b, TN)
    dup_ref[...] += dot(d_pre, norm_b, TN)


def attn_kernel(n_seq_tok, head_dim, n_alias, has_acc, *refs):
    y1_ref, y2_ref, dy1_ref, g_ref, dg_ref, ok_ref, qkv_ref, out_ref = refs[:8]
    refs = refs[8 + n_alias:]
    if has_acc:
        qkv_acc, out_acc = refs[:2]
        refs = refs[2:]
    x2_ref, dy1_out, branch_ref, dnorm_ref, dqkv_ref, dout_ref, qkv_t, out_t = refs
    score_scale = head_dim ** -0.5

    @pl.when(pl.program_id(0) == 0)
    def _():
        qkv_t[...] = qkv_ref[...].T
        out_t[...] = out_ref[...].T
        dqkv_ref[...] = qkv_acc[...] if has_acc else jnp.zeros_like(dqkv_ref)
        dout_ref[...] = out_acc[...] if has_acc else jnp.zeros_like(dout_ref)

    x_two = y2_ref[...] - g_ref[...]
    x2_ref[...] = x_two
    norm_b = rms_norm(x_two)[0].astype(BF16)
    normed, inv_rms = rms_norm(y1_ref[...])
    dy_one = dy1_ref[...] + rms_back(normed, inv_rms, dg_ref[...].astype(F32))
    dy1_out[...] = dy_one
    dy_b = dy_one.astype(BF16)

    qkv = dot(norm_b, qkv_t[...]).astype(BF16)
    d_attn = dot(dy_b, out_t[...]).astype(BF16)
    n_tok = qkv.shape[0]
    width = ok_ref.shape[-1]
    row_pos = lax.broadcasted_iota(jnp.int32, (width, width), 0)
    col_pos = lax.broadcasted_iota(jnp.int32, (width, width), 1)
    causal = (col_pos <= row_pos) & (row_pos // n_seq_tok == col_pos // n_seq_tok)
    attn_parts, dqkv_parts = [], []
    for part in range(n_tok // width):
        rows = slice(part * width, (part + 1) * width)
        query = qkv[rows, :head_dim]
        key = qkv[rows, head_dim:2 * head_dim]
        value = qkv[rows, 2 * head_dim:]
        d_out = d_attn[rows]
        visible = causal & (ok_ref[part] > 0.5)
        scores = jnp.where(visible, dot(query, key, NT) * score_scale, MASK_VALUE)
        expd = jnp.exp(scores - jnp.max(scores, axis=-1, keepdims=True))
        probs = expd / jnp.sum(expd, axis=-1, keepdims=True)
        probs_b = probs.astype(BF16)
        attn_parts.append(dot(probs_b, value).astype(BF16))
        d_value = dot(probs_b, d_out, TN).astype(BF16)
        d_probs = dot(d_out, value, NT)
        row_sum = jnp.sum(d_probs * probs, axis=-1, keepdims=True)
        d_scores = (probs * (d_probs - row_sum) * score_scale).astype(BF16)
        d_query = dot(d_scores, key).astype(BF16)
        d_key = dot(d_scores, query, TN).astype(BF16)
        dqkv_parts.append(jnp.concatenate([d_query, d_key, d_value], axis=1))
    attn = jnp.concatenate(attn_parts, axis=0)
    dqkv = jnp.concatenate(dqkv_parts, axis=0)
    branch_ref[...] = dot(attn, out_ref[...]).astype(BF16)
    dnorm_ref[...] = dot(dqkv, qkv_ref[...]).astype(BF16)
    dout_ref[...] += dot(attn, dy_b, TN)
    dqkv_ref[...] += dot(dqkv, norm_b, TN)


def widen_kernel(n_alias, *refs):
    x1_in, dx2_in = refs[:2]
    x1_ref, dx2_ref = refs[2 + n_alias:]
    x1_ref[...] = x1_in[...].astype(F32)
    dx2_ref[...] = dx2_in[...].astype(F32)


def tile_of(n_tok, want):
    tile = want
    while n_tok % tile:
        tile //= 2
    return tile


def shape_of(shape, dtype=F32):
    return jax.ShapeDtypeStruct(shape, dtype)


def params():
    return pltpu.CompilerParams(dimension_semantics=('arbitrary',), vmem_limit_bytes=VMEM_LIMIT)


def whole(arr):
    return pl.BlockSpec(arr.shape, lambda i: (0,) * len(arr.shape))


ANY = pl.BlockSpec(memory_space=pl.ANY)


def run_ffn(start, n_tok, y_one, dy_two, w_up, w_down, acc):
    width, cols = y_one.shape[1], w_up.shape[1]
    tile = tile_of(n_tok, 512)
    off = start // tile
    far = pl.BlockSpec((tile, width), lambda i: (off + i, 0))
    near = pl.BlockSpec((tile, width), lambda i: (i, 0))
    grad = pl.BlockSpec((cols, width), lambda i: (0, 0))
    return pl.pallas_call(
        functools.partial(ffn_kernel, acc is not None),
        grid=(n_tok // tile,),
        in_specs=[far, far, whole(w_up), whole(w_down)] + [grad] * (0 if acc is None else 2),
        out_specs=[near, near, grad, grad],
        out_shape=[shape_of((n_tok, width)), shape_of((n_tok, width), BF16)] + [shape_of((cols, width))] * 2,
        scratch_shapes=[pltpu.VMEM((cols, width), BF16), pltpu.VMEM((width, cols), BF16)],
        compiler_params=params(),
        cost_estimate=pl.CostEstimate(flops=12 * n_tok * width * cols, bytes_accessed=12 * n_tok * width,
                                      transcendentals=n_tok * cols),
        name='ffn',
    )(y_one, dy_two, w_up, w_down, *(acc or ()))


def run_attn(start, n_tok, seq_tok, head_dim, y_one, y_two, dy_one, g_sum, dg_sum, key_ok, w_qkv, w_out, prev, acc):
    n_all, width = y_one.shape
    tile = tile_of(n_tok, 256)
    off = start // tile
    far = pl.BlockSpec((tile, width), lambda i: (off + i, 0))
    near = pl.BlockSpec((tile, width), lambda i: (i, 0))
    group = key_ok.shape[-1]
    per_tile = tile // group
    ok_spec = pl.BlockSpec((per_tile, 1, group), lambda i: (off + i, 0, 0))
    n_alias = 0 if prev is None else 2
    grads = [whole(w_qkv), whole(w_out)]
    return pl.pallas_call(
        functools.partial(attn_kernel, seq_tok, head_dim, n_alias, acc is not None),
        grid=(n_tok // tile,),
        in_specs=[far, far, far, near, near, ok_spec] + grads + [ANY] * n_alias + (grads if acc is not None else []),
        out_specs=[far, far, near, near] + grads,
        out_shape=[shape_of((n_all, width))] * 2 + [shape_of((n_tok, width), BF16)] * 2
        + [shape_of(w_qkv.shape), shape_of(w_out.shape)],
        scratch_shapes=[pltpu.VMEM(w_qkv.shape[::-1], BF16), pltpu.VMEM(w_out.shape[::-1], BF16)],
        input_output_aliases={8 + k: k for k in range(n_alias)},
        compiler_params=params(),
        cost_estimate=pl.CostEstimate(flops=24 * n_tok * width * head_dim, bytes_accessed=28 * n_tok * width,
                                      transcendentals=n_tok * group),
        name='attn',
    )(y_one, y_two, dy_one, g_sum, dg_sum, key_ok, w_qkv, w_out, *(prev or ()), *(acc or ()))


def run_widen(start, n_all, x_one, dx_two, prev):
    n_tok, width = x_one.shape
    tile = tile_of(n_tok, 256)
    off = start // tile
    far = pl.BlockSpec((tile, width), lambda i: (off + i, 0))
    near = pl.BlockSpec((tile, width), lambda i: (i, 0))
    n_alias = 0 if prev is None else 2
    return pl.pallas_call(
        functools.partial(widen_kernel, n_alias),
        grid=(n_tok // tile,),
        in_specs=[near, near] + [ANY] * n_alias,
        out_specs=[far, far],
        out_shape=[shape_of((n_all, width))] * 2,
        input_output_aliases={2 + k: k for k in range(n_alias)},
        compiler_params=params(),
        cost_estimate=pl.CostEstimate(flops=16 * n_tok * width, bytes_accessed=12 * n_tok * width, transcendentals=0),
        name='widen',
    )(x_one, dx_two, *(prev or ()))


def split_tokens(n_seq, seq_tok):
    parts = N_CHUNKS
    while n_seq % parts:
        parts -= 1
    step = n_seq // parts * seq_tok
    return [(k * step, step) for k in range(parts)]


def block_back(carry, seq_lens, layer_w):
    y_one, y_two, dy_one, dy_two = carry
    w_query, w_key, w_value, w_out, w_up, w_down = layer_w
    n_seq, seq_tok = y_one.shape[:2]
    head_dim = w_query.shape[2]
    act_shape = y_one.shape
    y_one, y_two, dy_one, dy_two = (a.reshape(-1, a.shape[-1]) for a in carry)
    w_qkv = jnp.concatenate([w[:, 0, :].T for w in (w_query, w_key, w_value)], axis=0)
    wo_flat = w_out[0]
    chunks = split_tokens(n_seq, seq_tok)
    group = tile_of(chunks[0][1], 128)
    key_pos = lax.broadcasted_iota(jnp.int32, (n_seq, seq_tok), 1)
    key_ok = (key_pos < seq_lens[:, None]).astype(F32).reshape(-1, 1, group)

    rank = lax.axis_index('tp')

    def reduce_all(val, earlier):
        if earlier is not None:
            val = lax.optimization_barrier((val, earlier))[0]
        return lax.psum(val, 'tp')

    def reduce_rows(val):
        return lax.psum_scatter(val, 'tp', scatter_dimension=0, tiled=True)

    def gather_rows(val):
        return lax.all_gather(val, 'tp', axis=0, tiled=True)

    acc, g_parts = None, []
    for start, n_tok in chunks:
        g_part, dg_part, *acc = run_ffn(start, n_tok, y_one, dy_two, w_up, w_down, acc)
        g_parts.append((g_part, dg_part))
    dw_up, dw_down = acc[0].T, acc[1]
    g_sums, sums = [], (None, None)
    for pair in g_parts:
        sums = tuple(map(reduce_all, pair, sums))
        g_sums.append(sums)
    acc, state, f_parts = None, None, []
    for (start, n_tok), sums in zip(chunks, g_sums):
        outs = run_attn(start, n_tok, seq_tok, head_dim, y_one, y_two, dy_one, *sums, key_ok, w_qkv, wo_flat, state, acc)
        state, acc = outs[:2], outs[4:]
        f_parts.append(outs[2:4])
    x_two, dy_one_new = state
    dw_qkv, dw_out = acc
    state = None
    for (start, n_tok), parts in zip(chunks, f_parts):
        f_rows, df_rows = (reduce_rows(part).astype(F32) for part in parts)
        n_rows = f_rows.shape[0]
        y1_rows, x2_rows, dy2_rows = (lax.dynamic_slice_in_dim(arr, start + rank * n_rows, n_rows, 0)
                                      for arr in (y_one, x_two, dy_two))
        dx2_rows = dy2_rows + rms_back(*rms_norm(x2_rows), df_rows)
        ends = gather_rows((y1_rows - f_rows).astype(BF16)), gather_rows(dx2_rows.astype(BF16))
        state = run_widen(start, y_one.shape[0], *ends, state)
    x_one, dx_two = state
    dw_heads = [dw_qkv[k * head_dim:(k + 1) * head_dim].T[:, None, :] for k in range(3)]
    carry = tuple(a.reshape(act_shape) for a in (x_one, x_two, dy_one_new, dx_two))
    return carry, (*dw_heads, dw_out[None], dw_up, dw_down)


def stack_grads(grads_by_layer):
    return tuple(jnp.stack([layer_grads[grad_pos] for layer_grads in grads_by_layer]) for grad_pos in range(6))


def solution(mesh):
    act_spec = P('dp', None, None)
    w_specs = (P(None, None, 'tp', None), P(None, None, 'tp', None), P(None, None, 'tp', None),
               P(None, 'tp', None, None), P(None, None, 'tp'), P(None, 'tp', None))
    g_specs = (P('dp', None, 'tp', None), P('dp', None, 'tp', None), P('dp', None, 'tp', None),
               P('dp', 'tp', None, None), P('dp', None, 'tp'), P('dp', 'tp', None))

    def local_fn(y_one, y_two, dy_one, dy_two, seq_lens, w_query, w_key, w_value, w_out, w_up, w_down):
        weights = (w_query, w_key, w_value, w_out, w_up, w_down)
        carry = (y_one, y_two, dy_one, dy_two)
        n_layers = w_query.shape[0]
        grads_by_layer = [None] * n_layers
        for layer_idx in reversed(range(n_layers)):
            layer_w = tuple(w_stack[layer_idx] for w_stack in weights)
            carry, grads_by_layer[layer_idx] = block_back(carry, seq_lens, layer_w)
        return carry + stack_grads(grads_by_layer)

    return jax.shard_map(local_fn, mesh=mesh,
                         in_specs=(act_spec,) * 4 + (P('dp'),) + w_specs,
                         out_specs=(act_spec,) * 4 + g_specs,
                         check_vma=False)
```

```python
import functools

import jax
import jax.numpy as jnp
from jax import lax
from jax.experimental import pallas as pl
from jax.experimental.pallas import tpu as pltpu
from jax.sharding import PartitionSpec as P

F32 = jnp.float32
BF16 = jnp.bfloat16
EPS = 1e-5
MASK_VALUE = -1e30
GELU_COEF = 0.044715
GELU_SCALE = (2.0 / jnp.pi) ** 0.5
VMEM_LIMIT = 60 * 1024 * 1024
LANES = 128
MESH = pl.DeviceIdType.MESH
NN = (((1,), (0,)), ((), ()))
NT = (((1,), (1,)), ((), ()))
TN = (((0,), (0,)), ((), ()))


def dot(lhs, rhs, dims=NN):
    return lax.dot_general(lhs, rhs, dims, preferred_element_type=F32)


def rms_norm(x_val):
    inv_rms = lax.rsqrt(jnp.mean(x_val * x_val, axis=-1, keepdims=True) + EPS)
    return x_val * inv_rms, inv_rms


def rms_back(normed, inv_rms, grad_norm):
    return inv_rms * (grad_norm - normed * jnp.mean(grad_norm * normed, axis=-1, keepdims=True))


def gelu_and_slope(x_val):
    tanh_val = jnp.tanh(GELU_SCALE * (x_val + GELU_COEF * (x_val * x_val * x_val)))
    cdf = 0.5 * (1.0 + tanh_val)
    inner_slope = GELU_SCALE * (1.0 + 3.0 * GELU_COEF * (x_val * x_val))
    return x_val * cdf, cdf + x_val * (0.5 * (1.0 - tanh_val * tanh_val) * inner_slope)


def ffn_kernel(y_ref, dy_ref, up_ref, down_ref, branch_ref, dnorm_ref, dup_ref, ddown_ref, up_t, down_t):
    @pl.when(pl.program_id(0) == 0)
    def _():
        up_t[...] = up_ref[...].T
        down_t[...] = down_ref[...].T
        dup_ref[...] = jnp.zeros_like(dup_ref)
        ddown_ref[...] = jnp.zeros_like(ddown_ref)

    norm_b = rms_norm(y_ref[...])[0].astype(BF16)
    dy_b = dy_ref[...].astype(BF16)
    act_val, slope = gelu_and_slope(dot(norm_b, up_ref[...]))
    act_b = act_val.astype(BF16)
    branch_ref[...] = dot(act_b, down_ref[...])
    d_pre = (slope * dot(dy_b, down_t[...])).astype(BF16)
    dnorm_ref[...] = dot(d_pre, up_t[...]).astype(BF16)
    ddown_ref[...] += dot(act_b, dy_b, TN)
    dup_ref[...] += dot(d_pre, norm_b, TN)


def attn_kernel(n_seq_tok, head_dim, nf_ref, dy_ref, ok_ref, qkv_ref, out_ref,
                x2_ref, dy1_ref, branch_ref, dnorm_ref, dqkv_ref, dout_ref, qkv_t, out_t):
    score_scale = head_dim ** -0.5
    width = dy_ref.shape[1]

    @pl.when(pl.program_id(0) == 0)
    def _():
        qkv_t[...] = qkv_ref[...].T
        out_t[...] = out_ref[...].T
        dqkv_ref[...] = jnp.zeros_like(dqkv_ref)
        dout_ref[...] = jnp.zeros_like(dout_ref)

    norm_b = nf_ref[:, :width]
    scales = nf_ref[:, width:].astype(F32)
    x2_ref[...] = norm_b.astype(F32) * (scales[:, :1] + scales[:, LANES // 2:LANES // 2 + 1])
    dy_b = dy_ref[...]
    dy1_ref[...] = dy_b.astype(F32)

    qkv = dot(norm_b, qkv_t[...]).astype(BF16)
    d_attn = dot(dy_b, out_t[...]).astype(BF16)
    n_tok = qkv.shape[0]
    group = ok_ref.shape[-1]
    row_pos = lax.broadcasted_iota(jnp.int32, (group, group), 0)
    col_pos = lax.broadcasted_iota(jnp.int32, (group, group), 1)
    causal = (col_pos <= row_pos) & (row_pos // n_seq_tok == col_pos // n_seq_tok)
    attn_parts, dqkv_parts = [], []
    for part in range(n_tok // group):
        rows = slice(part * group, (part + 1) * group)
        query = qkv[rows, :head_dim]
        key = qkv[rows, head_dim:2 * head_dim]
        value = qkv[rows, 2 * head_dim:]
        d_out = d_attn[rows]
        visible = causal & (ok_ref[part] > 0.5)
        scores = jnp.where(visible, dot(query, key, NT) * score_scale, MASK_VALUE)
        expd = jnp.exp(scores - jnp.max(scores, axis=-1, keepdims=True))
        probs = expd / jnp.sum(expd, axis=-1, keepdims=True)
        probs_b = probs.astype(BF16)
        attn_parts.append(dot(probs_b, value).astype(BF16))
        d_value = dot(probs_b, d_out, TN).astype(BF16)
        d_probs = dot(d_out, value, NT)
        row_sum = jnp.sum(d_probs * probs, axis=-1, keepdims=True)
        d_scores = (probs * (d_probs - row_sum) * score_scale).astype(BF16)
        d_query = dot(d_scores, key).astype(BF16)
        d_key = dot(d_scores, query, TN).astype(BF16)
        dqkv_parts.append(jnp.concatenate([d_query, d_key, d_value], axis=1))
    attn = jnp.concatenate(attn_parts, axis=0)
    dqkv = jnp.concatenate(dqkv_parts, axis=0)
    branch_ref[...] = dot(attn, out_ref[...]).astype(BF16)
    dnorm_ref[...] = dot(dqkv, qkv_ref[...]).astype(BF16)
    dout_ref[...] += dot(attn, dy_b, TN)
    dqkv_ref[...] += dot(dqkv, norm_b, TN)


def widen_kernel(x1_in, dx2_in, x1_ref, dx2_ref):
    x1_ref[...] = x1_in[...].astype(F32)
    dx2_ref[...] = dx2_in[...].astype(F32)


def store_x2(total, rows, out, x2_out, at):
    x_two = rows['y_two'][at] - total[at]
    x2_out[at] = x_two
    normed, inv_rms = rms_norm(x_two)
    width = normed.shape[1]
    scale = jnp.broadcast_to(1.0 / inv_rms, (normed.shape[0], LANES))
    high = scale.astype(BF16).astype(F32)
    lane = lax.broadcasted_iota(jnp.int32, scale.shape, 1)
    out[at[0], :width] = normed.astype(BF16)
    out[at[0], width:] = jnp.where(lane < LANES // 2, high, scale - high).astype(BF16)


def store_dy1(total, rows, out, x2_out, at):
    out[at] = (rows['dy_one'][at] + rms_back(*rms_norm(rows['y_one'][at]), total[at])).astype(BF16)


def store_x1(total, rows, out, x2_out, at):
    out[at] = (rows['y_one'][at] - total[at]).astype(BF16)


def store_dx2(total, rows, out, x2_out, at):
    out[at] = (rows['dy_two'][at] + rms_back(*rms_norm(rows['x_two'][at]), total[at])).astype(BF16)


def exchange_kernel(side, row_names, stores, keeps_x2, *refs):
    n_row = len(row_names)
    parts, row_refs, refs = refs[:2], refs[2:2 + n_row], refs[2 + n_row:]
    outs, refs = refs[:2], refs[2:]
    x2_out = None
    if keeps_x2:
        x2_out, refs = refs[0], refs[1:]
    half, own, slot_a, slot_b, total, sent = (refs[2 * i:2 * i + 2] for i in range(6))
    refs = refs[12:]
    row_bufs, refs = dict(zip(row_names, refs[:n_row])), refs[n_row:]
    (pair_send, pair_recv, own_sem, a_send, a_recv, b_send, b_recv, row_sem, out_sem,
     c_send, c_recv, d_send, d_recv, e_send, e_recv) = refs
    steps = side - 1
    n_rows, width = total[0].shape
    quarter = width // 4

    me = lax.axis_index('tp')
    core = me % 2
    pos = {'x': (me // 2) % side, 'y': me // (2 * side)}
    partner = me + 1 - 2 * core
    other = {'x': 'y', 'y': 'x'}
    streams = (('x', 1), ('x', -1), ('y', 1), ('y', -1))

    def wrap(val):
        return (val + 2 * side) % side

    def device(axis, move):
        place = dict(pos)
        place[axis] = wrap(pos[axis] + move)
        return {'tp': (place['y'] * side + place['x']) * 2 + core}

    def cols(k, st):
        stop = (st + 1) * quarter if st < 3 else outs[k].shape[-1]
        return slice(st * quarter, stop)

    def line(ref, axis, block, *rest):
        return ref.at[(slice(None), block) + rest] if axis == 'x' else ref.at[(block, slice(None)) + rest]

    def remote(src, dst, send, recv, dev):
        return pltpu.make_async_remote_copy(src_ref=src, dst_ref=dst, send_sem=send, recv_sem=recv,
                                            device_id=dev, device_id_type=MESH)

    barrier = pltpu.get_barrier_semaphore()
    neighbours = [{'tp': partner}] + [device(axis, sign) for axis, sign in streams]
    for dev in neighbours:
        pl.semaphore_signal(barrier, inc=1, device_id=dev, device_id_type=MESH)

    row_copies = []
    for i, name in enumerate(row_names):
        src = row_refs[i] if name == 'x_two' else row_refs[i].at[pos['y'], pos['x'], core]
        row_copies.append(pltpu.make_async_copy(src, row_bufs[name], row_sem.at[i]))
        row_copies[-1].start()

    def own_copy(k, block):
        src = parts[k].at[block // side, block % side, core]
        return pltpu.make_async_copy(src, own[k].at[block % 2], own_sem.at[k, block % 2])

    for k in range(2):
        own_copy(k, 0).start()
    pl.semaphore_wait(barrier, len(neighbours))

    waits = []
    pair = {}
    for k in range(2):
        for row in range(side):
            pair[k, row] = remote(parts[k].at[row, :, 1 - core], half[k].at[row], pair_send.at[k, row],
                                  pair_recv.at[k, row], {'tp': partner})
            pair[k, row].start()
            waits.append(pair[k, row])

    def send_a(k, st, step):
        axis, sign = streams[st]
        if step == 0:
            src = line(half[k], axis, wrap(pos[axis] - sign), slice(None), slice(st * quarter, (st + 1) * quarter))
        else:
            src = slot_a[k].at[st, step - 1]
        copy = remote(src, slot_a[k].at[st, step], a_send.at[k, st, step], a_recv.at[k, st, step], device(axis, sign))
        copy.start()
        waits.append(copy)
        return copy

    def send_b(k, st, step):
        axis, sign = streams[st]
        axis = other[axis]
        if step == 0:
            src = slot_a[k].at[st, steps - 1, wrap(pos[axis] - sign)]
        else:
            src = slot_b[k].at[st, step - 1]
        copy = remote(src, slot_b[k].at[st, step], b_send.at[k, st, step], b_recv.at[k, st, step], device(axis, sign))
        copy.start()
        waits.append(copy)
        return copy

    going = {}
    for k in range(2):
        for block in range(side * side):
            row, col = block // side, block % side
            if block + 1 < side * side:
                own_copy(k, block + 1).start()
            if col == 0:
                pair[k, row].wait_recv()
            own_copy(k, block).wait()

            @pl.loop(0, n_rows // 16)
            def _(r, k=k, row=row, col=col, block=block):
                at = pl.ds(pl.multiple_of(r * 16, 16), 16)
                half[k][row, col, at] = (half[k][row, col, at].astype(F32)
                                         + own[k][block % 2, at].astype(F32)).astype(half[k].dtype)
        for st in range(4):
            going[k, st] = send_a(k, st, 0)

    for step in range(steps):
        for k in range(2):
            for st, (axis, sign) in enumerate(streams):
                going[k, st].wait_recv()
                mine = line(half[k], axis, wrap(pos[axis] - sign * (2 + step)), slice(None),
                            slice(st * quarter, (st + 1) * quarter))

                @pl.loop(0, side)
                def _(j, k=k, st=st, step=step, mine=mine):
                    slot_a[k][st, step, j] = (slot_a[k][st, step, j].astype(F32)
                                              + mine[j].astype(F32)).astype(slot_a[k].dtype)
                going[k, st] = send_a(k, st, step + 1) if step + 1 < steps else send_b(k, st, 0)

    for copy in row_copies:
        copy.wait()

    def gather_b(k, st, step):
        axis, sign = streams[st]
        axis = other[axis]
        at = dict(pos)
        at[axis] = wrap(pos[axis] - sign * step)
        block = outs[k].at[at['y'], at['x'], core, :, cols(k, st)]
        src = sent[k].at[:, cols(k, st)] if step == 0 else block
        copy = remote(src, block, c_send.at[k, st, step], c_recv.at[k, st, step], device(axis, sign))
        copy.start()
        waits.append(copy)
        return copy

    def gather_a(k, st, step):
        axis, sign = streams[st]
        group = line(outs[k], axis, wrap(pos[axis] - sign * step), core, slice(None), cols(k, st))
        if step < steps:
            copy = remote(group, group, d_send.at[k, st, step], d_recv.at[k, st, step], device(axis, sign))
            copy.start()
            waits.append(copy)
            going[k, st] = copy
        copy = remote(group, group, e_send.at[k, st, step], e_recv.at[k, st, step], {'tp': partner})
        copy.start()
        waits.append(copy)
        last.append(copy)

    last, out_copies = [], []
    for step in range(steps):
        for k in range(2):
            for st, (axis, sign) in enumerate(streams):
                going[k, st].wait_recv()
                mine = slot_a[k].at[st, steps - 1, wrap(pos[other[axis]] - sign * (2 + step))]
                if step + 1 < steps:
                    slot_b[k][st, step] = (slot_b[k][st, step].astype(F32) + mine[...].astype(F32)).astype(slot_b[k].dtype)
                    going[k, st] = send_b(k, st, step + 1)
                else:
                    total[k][:, st * quarter:(st + 1) * quarter] = slot_b[k][st, step].astype(F32) + mine[...].astype(F32)
            if step + 1 == steps:
                @pl.loop(0, n_rows // 16)
                def _(r, k=k):
                    at = (pl.ds(pl.multiple_of(r * 16, 16), 16), slice(0, width))
                    stores[k](total[k], row_bufs, sent[k], x2_out, at)
                out_copies.append(pltpu.make_async_copy(sent[k], outs[k].at[pos['y'], pos['x'], core], out_sem.at[k]))
                out_copies[-1].start()
                for st in range(4):
                    going[k, st] = gather_b(k, st, 0)

    for step in range(steps):
        for k in range(2):
            if step + 1 == steps:
                out_copies[k].wait()
            for st in range(4):
                going[k, st].wait_recv()
                if step + 1 < steps:
                    going[k, st] = gather_b(k, st, step + 1)
                else:
                    gather_a(k, st, 0)
    for step in range(steps):
        for k in range(2):
            for st in range(4):
                going[k, st].wait_recv()
                gather_a(k, st, step + 1)
    for copy in last:
        copy.wait_recv()
    for copy in waits:
        copy.wait_send()


def tile_of(n_tok, want):
    tile = want
    while n_tok % tile:
        tile //= 2
    return tile


def shape_of(shape, dtype=F32):
    return jax.ShapeDtypeStruct(shape, dtype)


def params():
    return pltpu.CompilerParams(dimension_semantics=('arbitrary',), vmem_limit_bytes=VMEM_LIMIT)


def whole(arr):
    return pl.BlockSpec(arr.shape, lambda i: (0,) * len(arr.shape))


ANY = pl.BlockSpec(memory_space=pl.ANY)


def run_ffn(y_one, dy_two, w_up, w_down):
    (n_tok, width), cols = y_one.shape, w_up.shape[1]
    tile = tile_of(n_tok, 512)
    rows = pl.BlockSpec((tile, width), lambda i: (i, 0))
    grad = pl.BlockSpec((cols, width), lambda i: (0, 0))
    return pl.pallas_call(
        ffn_kernel,
        grid=(n_tok // tile,),
        in_specs=[rows, rows, whole(w_up), whole(w_down)],
        out_specs=[rows, rows, grad, grad],
        out_shape=[shape_of((n_tok, width)), shape_of((n_tok, width), BF16)] + [shape_of((cols, width))] * 2,
        scratch_shapes=[pltpu.VMEM((cols, width), BF16), pltpu.VMEM((width, cols), BF16)],
        compiler_params=params(),
        cost_estimate=pl.CostEstimate(flops=12 * n_tok * width * cols, bytes_accessed=14 * n_tok * width,
                                      transcendentals=n_tok * cols),
        name='ffn',
    )(y_one, dy_two, w_up, w_down)


def run_attn(seq_tok, head_dim, norm_f, dy_one, key_ok, w_qkv, w_out):
    n_tok, width = dy_one.shape
    tile = tile_of(n_tok, 256)
    rows = pl.BlockSpec((tile, width), lambda i: (i, 0))
    group = key_ok.shape[-1]
    grads = [whole(w_qkv), whole(w_out)]
    return pl.pallas_call(
        functools.partial(attn_kernel, seq_tok, head_dim),
        grid=(n_tok // tile,),
        in_specs=[pl.BlockSpec((tile, norm_f.shape[1]), lambda i: (i, 0)), rows,
                  pl.BlockSpec((tile // group, 1, group), lambda i: (i, 0, 0))] + grads,
        out_specs=[rows, rows, rows, rows] + grads,
        out_shape=[shape_of((n_tok, width))] * 2 + [shape_of((n_tok, width), BF16)] * 2
        + [shape_of(w_qkv.shape), shape_of(w_out.shape)],
        scratch_shapes=[pltpu.VMEM(w_qkv.shape[::-1], BF16), pltpu.VMEM(w_out.shape[::-1], BF16)],
        compiler_params=params(),
        cost_estimate=pl.CostEstimate(flops=24 * n_tok * width * head_dim, bytes_accessed=16 * n_tok * width,
                                      transcendentals=n_tok * group),
        name='attn',
    )(norm_f, dy_one, key_ok, w_qkv, w_out)


def run_widen(x_one, dx_two):
    n_tok, width = x_one.shape
    tile = tile_of(n_tok, 256)
    rows = pl.BlockSpec((tile, width), lambda i: (i, 0))
    return pl.pallas_call(
        widen_kernel,
        grid=(n_tok // tile,),
        in_specs=[rows, rows],
        out_specs=[rows, rows],
        out_shape=[shape_of((n_tok, width))] * 2,
        compiler_params=params(),
        cost_estimate=pl.CostEstimate(flops=n_tok * width, bytes_accessed=12 * n_tok * width, transcendentals=0),
        name='widen',
    )(x_one, dx_two)


def run_exchange(n_dev, call_id, parts, row_arrays, stores, out_widths, keeps_x2, name):
    side = int(round((n_dev // 2) ** 0.5))
    n_tok, width = parts[0].shape
    n_rows = n_tok // n_dev
    quarter = width // 4

    def blocks(arr):
        return arr.reshape(side, side, 2, n_rows, arr.shape[1]) if arr.shape[0] == n_tok else arr

    outs = [shape_of((side, side, 2, n_rows, w), BF16) for w in out_widths]
    out_specs = [ANY] * 2
    if keeps_x2:
        outs.append(shape_of((n_rows, width)))
        out_specs.append(pl.BlockSpec(memory_space=pltpu.VMEM))
    kinds = [part.dtype for part in parts]
    scratch = [pltpu.VMEM((side, side, n_rows, width), kind) for kind in kinds]
    scratch += [pltpu.VMEM((2, n_rows, width), kind) for kind in kinds]
    scratch += [pltpu.VMEM((4, side - 1, side, n_rows, quarter), kind) for kind in kinds]
    scratch += [pltpu.VMEM((4, side - 1, n_rows, quarter), kind) for kind in kinds]
    scratch += [pltpu.VMEM((n_rows, width), F32)] * 2
    scratch += [pltpu.VMEM((n_rows, w), BF16) for w in out_widths]
    scratch += [pltpu.VMEM((n_rows, width), F32)] * len(row_arrays)
    dma = pltpu.SemaphoreType.DMA
    ring = dma((2, 4, side - 1))
    scratch += [dma((2, side))] * 2 + [dma((2, 2))] + [ring] * 4 + [dma((len(row_arrays),)), dma((2,))]
    scratch += [ring] * 4 + [dma((2, 4, side))] * 2
    gathered = pl.pallas_call(
        functools.partial(exchange_kernel, side, tuple(row_arrays), stores, keeps_x2),
        in_specs=[ANY] * (2 + len(row_arrays)),
        out_specs=out_specs,
        out_shape=outs,
        scratch_shapes=scratch,
        compiler_params=pltpu.CompilerParams(collective_id=call_id, has_side_effects=True,
                                             vmem_limit_bytes=VMEM_LIMIT),
        name=name,
    )(*map(blocks, parts), *map(blocks, row_arrays.values()))
    return [arr.reshape(-1, arr.shape[-1]) for arr in gathered]


def block_back(carry, seq_lens, layer_w, n_dev):
    w_query, w_key, w_value, w_out, w_up, w_down = layer_w
    act_shape = carry[0].shape
    n_seq, seq_tok, width = act_shape
    head_dim = w_query.shape[2]
    y_one, y_two, dy_one, dy_two = (a.reshape(-1, width) for a in carry)
    w_qkv = jnp.concatenate([w[:, 0, :].T for w in (w_query, w_key, w_value)], axis=0)
    group = tile_of(n_seq * seq_tok, 128)
    key_pos = lax.broadcasted_iota(jnp.int32, (n_seq, seq_tok), 1)
    key_ok = (key_pos < seq_lens[:, None]).astype(F32).reshape(-1, 1, group)

    g_part, dg_part, dw_up, dw_down = run_ffn(y_one, dy_two, w_up, w_down)
    norm_f, dy1_b, x2_rows = run_exchange(
        n_dev, 0, (g_part, dg_part), {'y_one': y_one, 'y_two': y_two, 'dy_one': dy_one},
        (store_x2, store_dy1), (width + LANES, width), True, 'exchange_g')
    x_two, dy_one, f_part, df_part, dw_qkv, dw_out = run_attn(seq_tok, head_dim, norm_f, dy1_b, key_ok, w_qkv, w_out[0])
    x1_b, dx2_b = run_exchange(
        n_dev, 1, (f_part, df_part), {'y_one': y_one, 'dy_two': dy_two, 'x_two': x2_rows},
        (store_x1, store_dx2), (width, width), False, 'exchange_f')
    x_one, dx_two = run_widen(x1_b, dx2_b)
    dw_heads = [dw_qkv[k * head_dim:(k + 1) * head_dim].T[:, None, :] for k in range(3)]
    carry = tuple(a.reshape(act_shape) for a in (x_one, x_two, dy_one, dx_two))
    return carry, (*dw_heads, dw_out[None], dw_up.T, dw_down)


def stack_grads(grads_by_layer):
    return tuple(jnp.stack([layer_grads[grad_pos] for layer_grads in grads_by_layer]) for grad_pos in range(6))


def solution(mesh):
    act_spec = P('dp', None, None)
    w_specs = (P(None, None, 'tp', None), P(None, None, 'tp', None), P(None, None, 'tp', None),
               P(None, 'tp', None, None), P(None, None, 'tp'), P(None, 'tp', None))
    g_specs = (P('dp', None, 'tp', None), P('dp', None, 'tp', None), P('dp', None, 'tp', None),
               P('dp', 'tp', None, None), P('dp', None, 'tp'), P('dp', 'tp', None))

    def local_fn(y_one, y_two, dy_one, dy_two, seq_lens, w_query, w_key, w_value, w_out, w_up, w_down):
        weights = (w_query, w_key, w_value, w_out, w_up, w_down)
        carry = (y_one, y_two, dy_one, dy_two)
        n_layers, n_dev = w_query.shape[0], mesh.shape['tp']
        grads_by_layer = [None] * n_layers
        for layer_idx in reversed(range(n_layers)):
            layer_w = tuple(w_stack[layer_idx] for w_stack in weights)
            carry, grads_by_layer[layer_idx] = block_back(carry, seq_lens, layer_w, n_dev)
        return carry + stack_grads(grads_by_layer)

    return jax.shard_map(local_fn, mesh=mesh,
                         in_specs=(act_spec,) * 4 + (P('dp'),) + w_specs,
                         out_specs=(act_spec,) * 4 + g_specs,
                         check_vma=False)
```

```python
import functools

import jax
import jax.numpy as jnp
from jax import lax
from jax.experimental import pallas as pl
from jax.experimental.pallas import tpu as pltpu
from jax.sharding import PartitionSpec as P

F32 = jnp.float32
BF16 = jnp.bfloat16
EPS = 1e-5
MASK_VALUE = -1e30
GELU_COEF = 0.044715
GELU_SCALE = (2.0 / jnp.pi) ** 0.5
VMEM_LIMIT = 60 * 1024 * 1024
LANES = 128
MESH = pl.DeviceIdType.MESH
NN = (((1,), (0,)), ((), ()))
NT = (((1,), (1,)), ((), ()))
TN = (((0,), (0,)), ((), ()))


def dot(lhs, rhs, dims=NN):
    return lax.dot_general(lhs, rhs, dims, preferred_element_type=F32)


def rms_norm(x_val):
    inv_rms = lax.rsqrt(jnp.mean(x_val * x_val, axis=-1, keepdims=True) + EPS)
    return x_val * inv_rms, inv_rms


def rms_back(normed, inv_rms, grad_norm):
    return inv_rms * (grad_norm - normed * jnp.mean(grad_norm * normed, axis=-1, keepdims=True))


def gelu_and_slope(x_val):
    tanh_val = jnp.tanh(GELU_SCALE * (x_val + GELU_COEF * (x_val * x_val * x_val)))
    cdf = 0.5 * (1.0 + tanh_val)
    inner_slope = GELU_SCALE * (1.0 + 3.0 * GELU_COEF * (x_val * x_val))
    return x_val * cdf, cdf + x_val * (0.5 * (1.0 - tanh_val * tanh_val) * inner_slope)


def ffn_kernel(y_ref, dy_ref, up_ref, down_ref, branch_ref, dnorm_ref, dup_ref, ddown_ref, up_t, down_t):
    @pl.when(pl.program_id(0) == 0)
    def _():
        up_t[...] = up_ref[...].T
        down_t[...] = down_ref[...].T
        dup_ref[...] = jnp.zeros_like(dup_ref)
        ddown_ref[...] = jnp.zeros_like(ddown_ref)

    norm_b = rms_norm(y_ref[...])[0].astype(BF16)
    dy_b = dy_ref[...].astype(BF16)
    act_val, slope = gelu_and_slope(dot(norm_b, up_ref[...]))
    act_b = act_val.astype(BF16)
    branch_ref[...] = dot(act_b, down_ref[...])
    d_pre = (slope * dot(dy_b, down_t[...])).astype(BF16)
    dnorm_ref[...] = dot(d_pre, up_t[...]).astype(BF16)
    ddown_ref[...] += dot(act_b, dy_b, TN)
    dup_ref[...] += dot(d_pre, norm_b, TN)


def attn_kernel(seq_tok, group, nf_ref, dy_ref, lens_ref, query_ref, key_ref, value_ref, out_ref, dup_ref,
                x2_ref, dy1_ref, branch_ref, dnorm_ref, dq_ref, dk_ref, dv_ref, dout_ref, dup_t, qkv, qkv_t, out_t):
    head_dim = query_ref.shape[0]
    score_scale = head_dim ** -0.5
    n_tok, width = dy_ref.shape
    grads = (dq_ref, dk_ref, dv_ref)

    @pl.when(pl.program_id(0) == 0)
    def _():
        for k, w_ref in enumerate((query_ref, key_ref, value_ref)):
            qkv[k * head_dim:(k + 1) * head_dim] = w_ref[...]
            grads[k][...] = jnp.zeros_like(grads[k])
        qkv_t[...] = qkv[...].T
        out_t[...] = out_ref[...].T
        dout_ref[...] = jnp.zeros_like(dout_ref)
        dup_t[...] = dup_ref[...].T

    norm_b = nf_ref[:, :width]
    scales = nf_ref[:, width:].astype(F32)
    x2_ref[...] = norm_b.astype(F32) * (scales[:, :1] + scales[:, LANES // 2:LANES // 2 + 1])
    dy_b = dy_ref[...]
    dy1_ref[...] = dy_b.astype(F32)

    proj = dot(norm_b, qkv_t[...]).astype(BF16)
    d_attn = dot(dy_b, out_t[...]).astype(BF16)
    row_pos = lax.broadcasted_iota(jnp.int32, (group, group), 0)
    col_pos = lax.broadcasted_iota(jnp.int32, (group, group), 1)
    causal = (col_pos <= row_pos) & (row_pos // seq_tok == col_pos // seq_tok)
    lane = lax.broadcasted_iota(jnp.int32, (1, group), 1)
    first_seq = pl.program_id(0) * (n_tok // seq_tok)
    attn_parts, dqkv_parts = [], []
    for part in range(n_tok // group):
        rows = slice(part * group, (part + 1) * group)
        query = proj[rows, :head_dim]
        key = proj[rows, head_dim:2 * head_dim]
        value = proj[rows, 2 * head_dim:]
        d_out = d_attn[rows]
        limit = jnp.zeros_like(lane)
        for seq in range(group // seq_tok):
            seq_len = lens_ref[first_seq + part * (group // seq_tok) + seq]
            limit = jnp.where(lane // seq_tok == seq, seq_len, limit)
        visible = causal & (lane % seq_tok < limit)
        scores = jnp.where(visible, dot(query, key, NT) * score_scale, MASK_VALUE)
        expd = jnp.exp(scores - jnp.max(scores, axis=-1, keepdims=True))
        probs = expd / jnp.sum(expd, axis=-1, keepdims=True)
        probs_b = probs.astype(BF16)
        attn_parts.append(dot(probs_b, value).astype(BF16))
        d_value = dot(probs_b, d_out, TN).astype(BF16)
        d_probs = dot(d_out, value, NT)
        row_sum = jnp.sum(d_probs * probs, axis=-1, keepdims=True)
        d_scores = (probs * (d_probs - row_sum) * score_scale).astype(BF16)
        d_query = dot(d_scores, key).astype(BF16)
        d_key = dot(d_scores, query, TN).astype(BF16)
        dqkv_parts.append(jnp.concatenate([d_query, d_key, d_value], axis=1))
    attn = jnp.concatenate(attn_parts, axis=0)
    dqkv = jnp.concatenate(dqkv_parts, axis=0)
    branch_ref[...] = dot(attn, out_ref[...]).astype(BF16)
    dnorm_ref[...] = dot(dqkv, qkv[...]).astype(BF16)
    dout_ref[...] += dot(attn, dy_b, TN)
    d_heads = dot(dqkv, norm_b, TN)
    for k, grad in enumerate(grads):
        grad[...] += d_heads[k * head_dim:(k + 1) * head_dim]


def widen_kernel(x1_in, dx2_in, x1_ref, dx2_ref):
    x1_ref[...] = x1_in[...].astype(F32)
    dx2_ref[...] = dx2_in[...].astype(F32)


def store_x2(total, rows, out, x2_out, at):
    x_two = rows['y_two'][at] - total[at]
    x2_out[at] = x_two
    normed, inv_rms = rms_norm(x_two)
    width = normed.shape[1]
    scale = jnp.broadcast_to(1.0 / inv_rms, (normed.shape[0], LANES))
    high = scale.astype(BF16).astype(F32)
    lane = lax.broadcasted_iota(jnp.int32, scale.shape, 1)
    out[at[0], :width] = normed.astype(BF16)
    out[at[0], width:] = jnp.where(lane < LANES // 2, high, scale - high).astype(BF16)


def store_dy1(total, rows, out, x2_out, at):
    out[at] = (rows['dy_one'][at] + rms_back(*rms_norm(rows['y_one'][at]), total[at])).astype(BF16)


def store_x1(total, rows, out, x2_out, at):
    out[at] = (rows['y_one'][at] - total[at]).astype(BF16)


def store_dx2(total, rows, out, x2_out, at):
    out[at] = (rows['dy_two'][at] + rms_back(*rms_norm(rows['x_two'][at]), total[at])).astype(BF16)


def exchange_kernel(side, row_names, stores, keeps_x2, *refs):
    n_row = len(row_names)
    parts, row_refs, refs = refs[:2], refs[2:2 + n_row], refs[2 + n_row:]
    outs, refs = refs[:2], refs[2:]
    x2_out = None
    if keeps_x2:
        x2_out, refs = refs[0], refs[1:]
    paired, own, slot_a, slot_b, total, sent = (refs[2 * i:2 * i + 2] for i in range(6))
    refs = refs[12:]
    row_bufs, refs = dict(zip(row_names, refs[:n_row])), refs[n_row:]
    (pair_send, pair_recv, own_sem, a_send, a_recv, b_send, b_recv, row_sem, out_sem,
     c_send, c_recv, d_send, d_recv, e_send, e_recv) = refs
    steps = side - 1
    n_rows, width = total[0].shape
    quarter = width // 4

    me = lax.axis_index('tp')
    core = me % 2
    pos = {'x': (me // 2) % side, 'y': me // (2 * side)}
    partner = me + 1 - 2 * core
    other = {'x': 'y', 'y': 'x'}
    streams = (('x', 1), ('x', -1), ('y', 1), ('y', -1))

    def wrap(val):
        return (val + 2 * side) % side

    def device(axis, move):
        place = dict(pos)
        place[axis] = wrap(pos[axis] + move)
        return {'tp': (place['y'] * side + place['x']) * 2 + core}

    def cols(k, st):
        stop = (st + 1) * quarter if st < 3 else outs[k].shape[-1]
        return slice(st * quarter, stop)

    def line(ref, axis, block, *rest):
        return ref.at[(slice(None), block) + rest] if axis == 'x' else ref.at[(block, slice(None)) + rest]

    def remote(src, dst, send, recv, dev):
        return pltpu.make_async_remote_copy(src_ref=src, dst_ref=dst, send_sem=send, recv_sem=recv,
                                            device_id=dev, device_id_type=MESH)

    barrier = pltpu.get_barrier_semaphore()
    neighbours = [{'tp': partner}] + [device(axis, sign) for axis, sign in streams]
    for dev in neighbours:
        pl.semaphore_signal(barrier, inc=1, device_id=dev, device_id_type=MESH)

    row_copies = []
    for i, name in enumerate(row_names):
        src = row_refs[i] if name == 'x_two' else row_refs[i].at[pos['y'], pos['x'], core]
        row_copies.append(pltpu.make_async_copy(src, row_bufs[name], row_sem.at[i]))
        row_copies[-1].start()

    def piece(k, st, turn, whose):
        axis, sign = streams[st]
        return line(parts[k], axis, wrap(pos[axis] - sign * (1 + turn)), whose, slice(None),
                    slice(st * quarter, (st + 1) * quarter))

    def own_copy(k, st, turn):
        return pltpu.make_async_copy(piece(k, st, turn, core), own[k].at[st], own_sem.at[k, st])

    for k in range(2):
        for st in range(4):
            own_copy(k, st, 0).start()
    pl.semaphore_wait(barrier, len(neighbours))

    waits = []
    pair = {}
    for turn in range(side):
        for k in range(2):
            for st in range(4):
                copy = remote(piece(k, st, turn, 1 - core), paired[k].at[st, turn], pair_send.at[k, st, turn],
                              pair_recv.at[k, st, turn], {'tp': partner})
                copy.start()
                pair[k, st, turn] = copy
                waits.append(copy)

    def send_a(k, st, step):
        axis, sign = streams[st]
        if step == 0:
            src = paired[k].at[st, 0]
        else:
            src = slot_a[k].at[st, step - 1]
        copy = remote(src, slot_a[k].at[st, step], a_send.at[k, st, step], a_recv.at[k, st, step], device(axis, sign))
        copy.start()
        waits.append(copy)
        return copy

    def send_b(k, st, step):
        axis, sign = streams[st]
        axis = other[axis]
        if step == 0:
            src = slot_a[k].at[st, steps - 1, wrap(pos[axis] - sign)]
        else:
            src = slot_b[k].at[st, step - 1]
        copy = remote(src, slot_b[k].at[st, step], b_send.at[k, st, step], b_recv.at[k, st, step], device(axis, sign))
        copy.start()
        waits.append(copy)
        return copy

    going = {}
    for turn in range(side):
        for k in range(2):
            for st in range(4):
                if turn:
                    going[k, st].wait_recv()
                pair[k, st, turn].wait_recv()
                own_copy(k, st, turn).wait()

                @pl.loop(0, side)
                def _(j, k=k, st=st, turn=turn):
                    mine = paired[k][st, turn, j].astype(F32) + own[k][st, j].astype(F32)
                    if turn:
                        slot_a[k][st, turn - 1, j] = (slot_a[k][st, turn - 1, j].astype(F32) + mine).astype(slot_a[k].dtype)
                    else:
                        paired[k][st, 0, j] = mine.astype(paired[k].dtype)

                if turn < steps:
                    own_copy(k, st, turn + 1).start()
                going[k, st] = send_a(k, st, turn) if turn < steps else send_b(k, st, 0)

    for copy in row_copies:
        copy.wait()

    def gather_b(k, st, step):
        axis, sign = streams[st]
        axis = other[axis]
        at = dict(pos)
        at[axis] = wrap(pos[axis] - sign * step)
        block = outs[k].at[at['y'], at['x'], core, :, cols(k, st)]
        src = sent[k].at[:, cols(k, st)] if step == 0 else block
        copy = remote(src, block, c_send.at[k, st, step], c_recv.at[k, st, step], device(axis, sign))
        copy.start()
        waits.append(copy)
        return copy

    def gather_a(k, st, step):
        axis, sign = streams[st]
        group = line(outs[k], axis, wrap(pos[axis] - sign * step), core, slice(None), cols(k, st))
        if step < steps:
            copy = remote(group, group, d_send.at[k, st, step], d_recv.at[k, st, step], device(axis, sign))
            copy.start()
            waits.append(copy)
            going[k, st] = copy
        copy = remote(group, group, e_send.at[k, st, step], e_recv.at[k, st, step], {'tp': partner})
        copy.start()
        waits.append(copy)
        last.append(copy)

    last, out_copies = [], []
    for step in range(steps):
        for k in range(2):
            for st, (axis, sign) in enumerate(streams):
                going[k, st].wait_recv()
                mine = slot_a[k].at[st, steps - 1, wrap(pos[other[axis]] - sign * (2 + step))]
                if step + 1 < steps:
                    slot_b[k][st, step] = (slot_b[k][st, step].astype(F32) + mine[...].astype(F32)).astype(slot_b[k].dtype)
                    going[k, st] = send_b(k, st, step + 1)
                else:
                    total[k][:, st * quarter:(st + 1) * quarter] = slot_b[k][st, step].astype(F32) + mine[...].astype(F32)
            if step + 1 == steps:
                @pl.loop(0, n_rows // 16)
                def _(r, k=k):
                    at = (pl.ds(pl.multiple_of(r * 16, 16), 16), slice(0, width))
                    stores[k](total[k], row_bufs, sent[k], x2_out, at)
                out_copies.append(pltpu.make_async_copy(sent[k], outs[k].at[pos['y'], pos['x'], core], out_sem.at[k]))
                out_copies[-1].start()
                for st in range(4):
                    going[k, st] = gather_b(k, st, 0)

    for step in range(steps):
        for k in range(2):
            if step + 1 == steps:
                out_copies[k].wait()
            for st in range(4):
                going[k, st].wait_recv()
                if step + 1 < steps:
                    going[k, st] = gather_b(k, st, step + 1)
                else:
                    gather_a(k, st, 0)
    for step in range(steps):
        for k in range(2):
            for st in range(4):
                going[k, st].wait_recv()
                gather_a(k, st, step + 1)
    for copy in last:
        copy.wait_recv()
    for copy in waits:
        copy.wait_send()


def tile_of(n_tok, want):
    tile = want
    while n_tok % tile:
        tile //= 2
    return tile


def shape_of(shape, dtype=F32):
    return jax.ShapeDtypeStruct(shape, dtype)


def params():
    return pltpu.CompilerParams(dimension_semantics=('arbitrary',), vmem_limit_bytes=VMEM_LIMIT)


def whole(arr):
    return pl.BlockSpec(arr.shape, lambda i: (0,) * len(arr.shape))


ANY = pl.BlockSpec(memory_space=pl.ANY)


def run_ffn(y_one, dy_two, w_up, w_down):
    (n_tok, width), cols = y_one.shape, w_up.shape[1]
    tile = tile_of(n_tok, 512)
    rows = pl.BlockSpec((tile, width), lambda i: (i, 0))
    grad = pl.BlockSpec((cols, width), lambda i: (0, 0))
    return pl.pallas_call(
        ffn_kernel,
        grid=(n_tok // tile,),
        in_specs=[rows, rows, whole(w_up), whole(w_down)],
        out_specs=[rows, rows, grad, grad],
        out_shape=[shape_of((n_tok, width)), shape_of((n_tok, width), BF16)] + [shape_of((cols, width))] * 2,
        scratch_shapes=[pltpu.VMEM((cols, width), BF16), pltpu.VMEM((width, cols), BF16)],
        compiler_params=params(),
        cost_estimate=pl.CostEstimate(flops=12 * n_tok * width * cols, bytes_accessed=14 * n_tok * width,
                                      transcendentals=n_tok * cols),
        name='ffn',
    )(y_one, dy_two, w_up, w_down)


def run_attn(seq_tok, norm_f, dy_one, seq_lens, w_heads, w_out, dw_up):
    n_tok, width = dy_one.shape
    head_dim = w_out.shape[0]
    tile = tile_of(n_tok, 256)
    group = tile_of(tile, 128)
    rows = pl.BlockSpec((tile, width), lambda i: (i, 0))
    grads = [whole(w) for w in w_heads] + [whole(w_out)]
    up_shape = dw_up.shape[::-1]
    return pl.pallas_call(
        functools.partial(attn_kernel, seq_tok, group),
        grid=(n_tok // tile,),
        in_specs=[pl.BlockSpec((tile, norm_f.shape[1]), lambda i: (i, 0)), rows,
                  pl.BlockSpec(memory_space=pltpu.SMEM)] + grads + [whole(dw_up)],
        out_specs=[rows, rows, rows, rows] + grads + [pl.BlockSpec(up_shape, lambda i: (0, 0))],
        out_shape=[shape_of((n_tok, width))] * 2 + [shape_of((n_tok, width), BF16)] * 2
        + [shape_of(w_out.shape)] * 4 + [shape_of(up_shape)],
        scratch_shapes=[pltpu.VMEM((3 * head_dim, width), BF16), pltpu.VMEM((width, 3 * head_dim), BF16),
                        pltpu.VMEM((width, head_dim), BF16)],
        compiler_params=params(),
        cost_estimate=pl.CostEstimate(flops=24 * n_tok * width * head_dim, bytes_accessed=16 * n_tok * width,
                                      transcendentals=n_tok * group),
        name='attn',
    )(norm_f, dy_one, seq_lens, *w_heads, w_out, dw_up)


def run_widen(x_one, dx_two):
    n_tok, width = x_one.shape
    tile = tile_of(n_tok, 384)
    rows = pl.BlockSpec((tile, width), lambda i: (i, 0))
    return pl.pallas_call(
        widen_kernel,
        grid=(n_tok // tile,),
        in_specs=[rows, rows],
        out_specs=[rows, rows],
        out_shape=[shape_of((n_tok, width))] * 2,
        compiler_params=params(),
        cost_estimate=pl.CostEstimate(flops=n_tok * width, bytes_accessed=12 * n_tok * width, transcendentals=0),
        name='widen',
    )(x_one, dx_two)


def run_exchange(n_dev, call_id, parts, row_arrays, stores, out_widths, keeps_x2, name):
    side = int(round((n_dev // 2) ** 0.5))
    n_tok, width = parts[0].shape
    n_rows = n_tok // n_dev
    quarter = width // 4

    def blocks(arr):
        return arr.reshape(side, side, 2, n_rows, arr.shape[1]) if arr.shape[0] == n_tok else arr

    outs = [shape_of((side, side, 2, n_rows, w), BF16) for w in out_widths]
    out_specs = [ANY] * 2
    if keeps_x2:
        outs.append(shape_of((n_rows, width)))
        out_specs.append(pl.BlockSpec(memory_space=pltpu.VMEM))
    kinds = [part.dtype for part in parts]
    scratch = [pltpu.VMEM((4, side, side, n_rows, quarter), kind) for kind in kinds]
    scratch += [pltpu.VMEM((4, side, n_rows, quarter), kind) for kind in kinds]
    scratch += [pltpu.VMEM((4, side - 1, side, n_rows, quarter), kind) for kind in kinds]
    scratch += [pltpu.VMEM((4, side - 1, n_rows, quarter), kind) for kind in kinds]
    scratch += [pltpu.VMEM((n_rows, width), F32)] * 2
    scratch += [pltpu.VMEM((n_rows, w), BF16) for w in out_widths]
    scratch += [pltpu.VMEM((n_rows, width), F32)] * len(row_arrays)
    dma = pltpu.SemaphoreType.DMA
    ring = dma((2, 4, side - 1))
    scratch += [dma((2, 4, side))] * 2 + [dma((2, 4))] + [ring] * 4 + [dma((len(row_arrays),)), dma((2,))]
    scratch += [ring] * 4 + [dma((2, 4, side))] * 2
    gathered = pl.pallas_call(
        functools.partial(exchange_kernel, side, tuple(row_arrays), stores, keeps_x2),
        in_specs=[ANY] * (2 + len(row_arrays)),
        out_specs=out_specs,
        out_shape=outs,
        scratch_shapes=scratch,
        compiler_params=pltpu.CompilerParams(collective_id=call_id, has_side_effects=True,
                                             vmem_limit_bytes=VMEM_LIMIT),
        name=name,
    )(*map(blocks, parts), *map(blocks, row_arrays.values()))
    return [arr.reshape(-1, arr.shape[-1]) for arr in gathered]


def block_back(carry, seq_lens, layer_w, n_dev):
    w_query, w_key, w_value, w_out, w_up, w_down = layer_w
    act_shape = carry[0].shape
    seq_tok, width = act_shape[1:]
    y_one, y_two, dy_one, dy_two = (a.reshape(-1, width) for a in carry)
    w_heads = [w[:, 0, :].T for w in (w_query, w_key, w_value)]

    g_part, dg_part, dw_up, dw_down = run_ffn(y_one, dy_two, w_up, w_down)
    dy1_b, norm_f, x2_rows = run_exchange(
        n_dev, 0, (dg_part, g_part), {'y_one': y_one, 'y_two': y_two, 'dy_one': dy_one},
        (store_dy1, store_x2), (width, width + LANES), True, 'exchange_g')
    x_two, dy_one, f_part, df_part, *dw_heads, dw_out, dw_up = run_attn(
        seq_tok, norm_f, dy1_b, seq_lens, w_heads, w_out[0], dw_up)
    x1_b, dx2_b = run_exchange(
        n_dev, 1, (f_part, df_part), {'y_one': y_one, 'dy_two': dy_two, 'x_two': x2_rows},
        (store_x1, store_dx2), (width, width), False, 'exchange_f')
    x_one, dx_two = run_widen(x1_b, dx2_b)
    dw_heads = [dw.T[:, None, :] for dw in dw_heads]
    carry = tuple(a.reshape(act_shape) for a in (x_one, x_two, dy_one, dx_two))
    return carry, (*dw_heads, dw_out[None], dw_up, dw_down)


def stack_grads(grads_by_layer):
    return tuple(jnp.stack([layer_grads[grad_pos] for layer_grads in grads_by_layer]) for grad_pos in range(6))


def solution(mesh):
    act_spec = P('dp', None, None)
    w_specs = (P(None, None, 'tp', None), P(None, None, 'tp', None), P(None, None, 'tp', None),
               P(None, 'tp', None, None), P(None, None, 'tp'), P(None, 'tp', None))
    g_specs = (P('dp', None, 'tp', None), P('dp', None, 'tp', None), P('dp', None, 'tp', None),
               P('dp', 'tp', None, None), P('dp', None, 'tp'), P('dp', 'tp', None))

    def local_fn(y_one, y_two, dy_one, dy_two, seq_lens, w_query, w_key, w_value, w_out, w_up, w_down):
        weights = (w_query, w_key, w_value, w_out, w_up, w_down)
        carry = (y_one, y_two, dy_one, dy_two)
        n_layers, n_dev = w_query.shape[0], mesh.shape['tp']
        grads_by_layer = [None] * n_layers
        for layer_idx in reversed(range(n_layers)):
            layer_w = tuple(w_stack[layer_idx] for w_stack in weights)
            carry, grads_by_layer[layer_idx] = block_back(carry, seq_lens, layer_w, n_dev)
        return carry + stack_grads(grads_by_layer)

    return jax.shard_map(local_fn, mesh=mesh,
                         in_specs=(act_spec,) * 4 + (P('dp'),) + w_specs,
                         out_specs=(act_spec,) * 4 + g_specs,
                         check_vma=False)
```

```python
import functools

import jax
import jax.numpy as jnp
from jax import lax
from jax.experimental import pallas as pl
from jax.experimental.pallas import tpu as pltpu
from jax.sharding import PartitionSpec as P

F32 = jnp.float32
BF16 = jnp.bfloat16
EPS = 1e-5
MASK_VALUE = -1e30
GELU_COEF = 0.044715
GELU_SCALE = (2.0 / jnp.pi) ** 0.5
VMEM_LIMIT = 60 * 1024 * 1024
LANES = 128
MESH = pl.DeviceIdType.MESH
NN = (((1,), (0,)), ((), ()))
NT = (((1,), (1,)), ((), ()))
TN = (((0,), (0,)), ((), ()))


def dot(lhs, rhs, dims=NN):
    return lax.dot_general(lhs, rhs, dims, preferred_element_type=F32)


def rms_norm(x_val):
    inv_rms = lax.rsqrt(jnp.mean(x_val * x_val, axis=-1, keepdims=True) + EPS)
    return x_val * inv_rms, inv_rms


def rms_back(normed, inv_rms, grad_norm):
    return inv_rms * (grad_norm - normed * jnp.mean(grad_norm * normed, axis=-1, keepdims=True))


def gelu_and_slope(x_val):
    tanh_val = jnp.tanh(GELU_SCALE * (x_val + GELU_COEF * (x_val * x_val * x_val)))
    cdf = 0.5 * (1.0 + tanh_val)
    inner_slope = GELU_SCALE * (1.0 + 3.0 * GELU_COEF * (x_val * x_val))
    return x_val * cdf, cdf + x_val * (0.5 * (1.0 - tanh_val * tanh_val) * inner_slope)


def ffn_kernel(y_ref, dy_ref, up_ref, down_ref, branch_ref, dnorm_ref, dup_ref, ddown_ref, up_t, down_t):
    @pl.when(pl.program_id(0) == 0)
    def _():
        up_t[...] = up_ref[...].T
        down_t[...] = down_ref[...].T
        dup_ref[...] = jnp.zeros_like(dup_ref)
        ddown_ref[...] = jnp.zeros_like(ddown_ref)

    norm_b = rms_norm(y_ref[...])[0].astype(BF16)
    dy_b = dy_ref[...].astype(BF16)
    act_val, slope = gelu_and_slope(dot(norm_b, up_ref[...]))
    act_b = act_val.astype(BF16)
    branch_ref[...] = dot(act_b, down_ref[...]).astype(BF16)
    d_pre = (slope * dot(dy_b, down_t[...])).astype(BF16)
    dnorm_ref[...] = dot(d_pre, up_t[...]).astype(BF16)
    ddown_ref[...] += dot(act_b, dy_b, TN)
    dup_ref[...] += dot(d_pre, norm_b, TN)


def attn_kernel(seq_tok, group, n_rows, nf_ref, dy_ref, scale_ref, lens_ref, query_ref, key_ref, value_ref, out_ref, dup_ref,
                x2_ref, dy1_ref, branch_ref, dnorm_ref, dq_ref, dk_ref, dv_ref, dout_ref, dup_t, qkv, qkv_t, out_t):
    head_dim = query_ref.shape[0]
    score_scale = head_dim ** -0.5
    n_tok, width = dy_ref.shape
    grads = (dq_ref, dk_ref, dv_ref)

    @pl.when(pl.program_id(0) == 0)
    def _():
        for k, w_ref in enumerate((query_ref, key_ref, value_ref)):
            qkv[k * head_dim:(k + 1) * head_dim] = w_ref[...]
            grads[k][...] = jnp.zeros_like(grads[k])
        qkv_t[...] = qkv[...].T
        out_t[...] = out_ref[...].T
        dout_ref[...] = jnp.zeros_like(dout_ref)
        dup_t[...] = dup_ref[...].T

    norm_b = nf_ref[...]
    row = lax.broadcasted_iota(jnp.int32, (n_rows, LANES), 0)
    own_lane = lax.broadcasted_iota(jnp.int32, (n_rows, LANES), 1) == row
    for block in range(n_tok // n_rows):
        scales = scale_ref[block * 16:(block + 1) * 16].astype(F32)
        scale = jnp.where(own_lane, scales[:1] + scales[1:2], 0.0)
        at = slice(block * n_rows, (block + 1) * n_rows)
        x2_ref[at] = norm_b[at].astype(F32) * jnp.sum(scale, axis=1, keepdims=True)
    dy_b = dy_ref[...]
    dy1_ref[...] = dy_b.astype(F32)

    proj = dot(norm_b, qkv_t[...]).astype(BF16)
    d_attn = dot(dy_b, out_t[...]).astype(BF16)
    row_pos = lax.broadcasted_iota(jnp.int32, (group, group), 0)
    col_pos = lax.broadcasted_iota(jnp.int32, (group, group), 1)
    causal = (col_pos <= row_pos) & (row_pos // seq_tok == col_pos // seq_tok)
    lane = lax.broadcasted_iota(jnp.int32, (1, group), 1)
    first_seq = pl.program_id(0) * (n_tok // seq_tok)
    attn_parts, dqkv_parts = [], []
    for part in range(n_tok // group):
        rows = slice(part * group, (part + 1) * group)
        query = proj[rows, :head_dim]
        key = proj[rows, head_dim:2 * head_dim]
        value = proj[rows, 2 * head_dim:]
        d_out = d_attn[rows]
        limit = jnp.zeros_like(lane)
        for seq in range(group // seq_tok):
            seq_len = lens_ref[first_seq + part * (group // seq_tok) + seq]
            limit = jnp.where(lane // seq_tok == seq, seq_len, limit)
        visible = causal & (lane % seq_tok < limit)
        scores = jnp.where(visible, dot(query, key, NT) * score_scale, MASK_VALUE)
        expd = jnp.exp(scores - jnp.max(scores, axis=-1, keepdims=True))
        probs = expd / jnp.sum(expd, axis=-1, keepdims=True)
        probs_b = probs.astype(BF16)
        attn_parts.append(dot(probs_b, value).astype(BF16))
        d_value = dot(probs_b, d_out, TN).astype(BF16)
        d_probs = dot(d_out, value, NT)
        row_sum = jnp.sum(d_probs * probs, axis=-1, keepdims=True)
        d_scores = (probs * (d_probs - row_sum) * score_scale).astype(BF16)
        d_query = dot(d_scores, key).astype(BF16)
        d_key = dot(d_scores, query, TN).astype(BF16)
        dqkv_parts.append(jnp.concatenate([d_query, d_key, d_value], axis=1))
    attn = jnp.concatenate(attn_parts, axis=0)
    dqkv = jnp.concatenate(dqkv_parts, axis=0)
    branch_ref[...] = dot(attn, out_ref[...]).astype(BF16)
    dnorm_ref[...] = dot(dqkv, qkv[...]).astype(BF16)
    dout_ref[...] += dot(attn, dy_b, TN)
    d_heads = dot(dqkv, norm_b, TN)
    for k, grad in enumerate(grads):
        grad[...] += d_heads[k * head_dim:(k + 1) * head_dim]


def widen_kernel(x1_in, dx2_in, x1_ref, dx2_ref):
    x1_ref[...] = x1_in[...].astype(F32)
    dx2_ref[...] = dx2_in[...].astype(F32)


def store_x2(total, rows, out, x2_out, scale_buf, at):
    x_two = rows['y_two'][at] - total[at]
    x2_out[at] = x_two
    normed, inv_rms = rms_norm(x_two)
    out[at] = normed.astype(BF16)
    scale_buf[at[0]] = jnp.broadcast_to(1.0 / inv_rms, (normed.shape[0], LANES))


def pack_scales(scale_buf, out):
    n_rows = scale_buf.shape[0]
    row = lax.broadcasted_iota(jnp.int32, (n_rows, LANES), 0)
    lane = lax.broadcasted_iota(jnp.int32, (n_rows, LANES), 1)
    scale = jnp.sum(jnp.where(row == lane, scale_buf[...], 0.0), axis=0, keepdims=True)
    high = scale.astype(BF16).astype(F32)
    part = lax.broadcasted_iota(jnp.int32, out.shape, 0)
    out[...] = jnp.where(part == 0, high, scale - high).astype(BF16)


def store_dy1(total, rows, out, x2_out, scale_buf, at):
    out[at] = (rows['dy_one'][at] + rms_back(*rms_norm(rows['y_one'][at]), total[at])).astype(BF16)


def store_x1(total, rows, out, x2_out, scale_buf, at):
    out[at] = (rows['y_one'][at] - total[at]).astype(BF16)


def store_dx2(total, rows, out, x2_out, scale_buf, at):
    out[at] = (rows['dy_two'][at] + rms_back(*rms_norm(rows['x_two'][at]), total[at])).astype(BF16)


def exchange_kernel(side, row_names, stores, keeps_x2, *refs):
    n_row = len(row_names)
    parts, row_refs, refs = refs[:2], refs[2:2 + n_row], refs[2 + n_row:]
    n_out = 3 if keeps_x2 else 2
    outs, refs = refs[:n_out], refs[n_out:]
    x2_out = scale_buf = None
    if keeps_x2:
        x2_out, refs = refs[0], refs[1:]
    paired, own, slot_a, slot_b, total, sent = (refs[2 * i:2 * i + 2] for i in range(6))
    refs = refs[12:]
    if keeps_x2:
        sent, scale_buf, refs = (*sent, refs[0]), refs[1], refs[2:]
    row_bufs, refs = dict(zip(row_names, refs[:n_row])), refs[n_row:]
    (pair_send, pair_recv, own_sem, a_send, a_recv, b_send, b_recv, row_sem, out_sem,
     c_send, c_recv, d_send, d_recv, e_send, e_recv) = refs
    steps = side - 1
    n_rows, width = total[0].shape
    quarter = width // 4

    me = lax.axis_index('tp')
    core = me % 2
    pos = {'x': (me // 2) % side, 'y': me // (2 * side)}
    partner = me + 1 - 2 * core
    other = {'x': 'y', 'y': 'x'}
    streams = (('x', 1), ('x', -1), ('y', 1), ('y', -1))

    def wrap(val):
        return (val + 2 * side) % side

    def device(axis, move):
        place = dict(pos)
        place[axis] = wrap(pos[axis] + move)
        return {'tp': (place['y'] * side + place['x']) * 2 + core}

    def cols(k, st):
        return slice(st * quarter, (st + 1) * quarter) if k < 2 else slice(None)

    def lanes(k):
        return range(4 if k < 2 else 1)

    def line(ref, axis, block, *rest):
        return ref.at[(slice(None), block) + rest] if axis == 'x' else ref.at[(block, slice(None)) + rest]

    def remote(src, dst, send, recv, dev):
        return pltpu.make_async_remote_copy(src_ref=src, dst_ref=dst, send_sem=send, recv_sem=recv,
                                            device_id=dev, device_id_type=MESH)

    barrier = pltpu.get_barrier_semaphore()
    neighbours = [{'tp': partner}] + [device(axis, sign) for axis, sign in streams]
    for dev in neighbours:
        pl.semaphore_signal(barrier, inc=1, device_id=dev, device_id_type=MESH)

    row_copies = []
    for i, name in enumerate(row_names):
        src = row_refs[i] if name == 'x_two' else row_refs[i].at[pos['y'], pos['x'], core]
        row_copies.append(pltpu.make_async_copy(src, row_bufs[name], row_sem.at[i]))
        row_copies[-1].start()

    def piece(k, st, turn, whose):
        axis, sign = streams[st]
        return line(parts[k], axis, wrap(pos[axis] - sign * (1 + turn)), whose, slice(None),
                    slice(st * quarter, (st + 1) * quarter))

    def own_copy(k, st, turn):
        return pltpu.make_async_copy(piece(k, st, turn, core), own[k].at[st], own_sem.at[k, st])

    for k in range(2):
        for st in range(4):
            own_copy(k, st, 0).start()
    pl.semaphore_wait(barrier, len(neighbours))

    waits = []
    pair = {}
    for turn in range(side):
        for k in range(2):
            for st in range(4):
                copy = remote(piece(k, st, turn, 1 - core), paired[k].at[st, turn], pair_send.at[k, st, turn],
                              pair_recv.at[k, st, turn], {'tp': partner})
                copy.start()
                pair[k, st, turn] = copy
                waits.append(copy)

    def send_a(k, st, step):
        axis, sign = streams[st]
        if step == 0:
            src = paired[k].at[st, 0]
        else:
            src = slot_a[k].at[st, step - 1]
        copy = remote(src, slot_a[k].at[st, step], a_send.at[k, st, step], a_recv.at[k, st, step], device(axis, sign))
        copy.start()
        waits.append(copy)
        return copy

    def send_b(k, st, step):
        axis, sign = streams[st]
        axis = other[axis]
        if step == 0:
            src = slot_a[k].at[st, steps - 1, wrap(pos[axis] - sign)]
        else:
            src = slot_b[k].at[st, step - 1]
        copy = remote(src, slot_b[k].at[st, step], b_send.at[k, st, step], b_recv.at[k, st, step], device(axis, sign))
        copy.start()
        waits.append(copy)
        return copy

    going = {}
    for turn in range(side):
        for k in range(2):
            for st in range(4):
                if turn:
                    going[k, st].wait_recv()
                pair[k, st, turn].wait_recv()
                own_copy(k, st, turn).wait()

                @pl.loop(0, side)
                def _(j, k=k, st=st, turn=turn):
                    mine = paired[k][st, turn, j].astype(F32) + own[k][st, j].astype(F32)
                    if turn:
                        slot_a[k][st, turn - 1, j] = (slot_a[k][st, turn - 1, j].astype(F32) + mine).astype(slot_a[k].dtype)
                    else:
                        paired[k][st, 0, j] = mine.astype(paired[k].dtype)

                if turn < steps:
                    own_copy(k, st, turn + 1).start()
                going[k, st] = send_a(k, st, turn) if turn < steps else send_b(k, st, 0)

    for copy in row_copies:
        copy.wait()

    def gather_b(k, st, step):
        axis, sign = streams[st]
        axis = other[axis]
        at = dict(pos)
        at[axis] = wrap(pos[axis] - sign * step)
        block = outs[k].at[at['y'], at['x'], core, :, cols(k, st)]
        src = sent[k].at[:, cols(k, st)] if step == 0 else block
        copy = remote(src, block, c_send.at[k, st, step], c_recv.at[k, st, step], device(axis, sign))
        copy.start()
        waits.append(copy)
        return copy

    def gather_a(k, st, step):
        axis, sign = streams[st]
        group = line(outs[k], axis, wrap(pos[axis] - sign * step), core, slice(None), cols(k, st))
        if step < steps:
            copy = remote(group, group, d_send.at[k, st, step], d_recv.at[k, st, step], device(axis, sign))
            copy.start()
            waits.append(copy)
            going[k, st] = copy
        copy = remote(group, group, e_send.at[k, st, step], e_recv.at[k, st, step], {'tp': partner})
        copy.start()
        waits.append(copy)
        last.append(copy)

    last, out_copies = [], []
    for step in range(steps):
        for k in range(2):
            for st, (axis, sign) in enumerate(streams):
                going[k, st].wait_recv()
                mine = slot_a[k].at[st, steps - 1, wrap(pos[other[axis]] - sign * (2 + step))]
                if step + 1 < steps:
                    slot_b[k][st, step] = (slot_b[k][st, step].astype(F32) + mine[...].astype(F32)).astype(slot_b[k].dtype)
                    going[k, st] = send_b(k, st, step + 1)
                else:
                    total[k][:, st * quarter:(st + 1) * quarter] = slot_b[k][st, step].astype(F32) + mine[...].astype(F32)
            if step + 1 == steps:
                @pl.loop(0, n_rows // 16)
                def _(r, k=k):
                    at = (pl.ds(pl.multiple_of(r * 16, 16), 16), slice(0, width))
                    stores[k](total[k], row_bufs, sent[k], x2_out, scale_buf, at)
                ready = [k]
                if k == 1 and n_out == 3:
                    pack_scales(scale_buf, sent[2])
                    ready.append(2)
                for i in ready:
                    out_copies.append(pltpu.make_async_copy(sent[i], outs[i].at[pos['y'], pos['x'], core], out_sem.at[i]))
                    out_copies[-1].start()
                    for st in lanes(i):
                        going[i, st] = gather_b(i, st, 0)

    for step in range(steps):
        for k in range(n_out):
            if step + 1 == steps:
                out_copies[k].wait()
            for st in lanes(k):
                going[k, st].wait_recv()
                if step + 1 < steps:
                    going[k, st] = gather_b(k, st, step + 1)
                else:
                    gather_a(k, st, 0)
    for step in range(steps):
        for k in range(n_out):
            for st in lanes(k):
                going[k, st].wait_recv()
                gather_a(k, st, step + 1)
    for copy in last:
        copy.wait_recv()
    for copy in waits:
        copy.wait_send()


def tile_of(n_tok, want):
    tile = want
    while n_tok % tile:
        tile //= 2
    return tile


def shape_of(shape, dtype=F32):
    return jax.ShapeDtypeStruct(shape, dtype)


def params():
    return pltpu.CompilerParams(dimension_semantics=('arbitrary',), vmem_limit_bytes=VMEM_LIMIT)


def whole(arr):
    return pl.BlockSpec(arr.shape, lambda i: (0,) * len(arr.shape))


ANY = pl.BlockSpec(memory_space=pl.ANY)


def run_ffn(y_one, dy_two, w_up, w_down):
    (n_tok, width), cols = y_one.shape, w_up.shape[1]
    tile = tile_of(n_tok, 256)
    rows = pl.BlockSpec((tile, width), lambda i: (i, 0))
    grad = pl.BlockSpec((cols, width), lambda i: (0, 0))
    return pl.pallas_call(
        ffn_kernel,
        grid=(n_tok // tile,),
        in_specs=[rows, rows, whole(w_up), whole(w_down)],
        out_specs=[rows, rows, grad, grad],
        out_shape=[shape_of((n_tok, width), BF16)] * 2 + [shape_of((cols, width))] * 2,
        scratch_shapes=[pltpu.VMEM((cols, width), BF16), pltpu.VMEM((width, cols), BF16)],
        compiler_params=params(),
        cost_estimate=pl.CostEstimate(flops=12 * n_tok * width * cols, bytes_accessed=14 * n_tok * width,
                                      transcendentals=n_tok * cols),
        name='ffn',
    )(y_one, dy_two, w_up, w_down)


def run_attn(seq_tok, norm_f, dy_one, scales, seq_lens, w_heads, w_out, dw_up):
    n_tok, width = dy_one.shape
    head_dim = w_out.shape[0]
    n_rows = n_tok * 16 // scales.shape[0]
    tile = 4 * n_rows
    group = tile_of(tile, 128)
    rows = pl.BlockSpec((tile, width), lambda i: (i, 0))
    grads = [whole(w) for w in w_heads] + [whole(w_out)]
    up_shape = dw_up.shape[::-1]
    return pl.pallas_call(
        functools.partial(attn_kernel, seq_tok, group, n_rows),
        grid=(n_tok // tile,),
        in_specs=[rows, rows, pl.BlockSpec((tile // n_rows * 16, LANES), lambda i: (i, 0)),
                  pl.BlockSpec(memory_space=pltpu.SMEM)] + grads + [whole(dw_up)],
        out_specs=[rows, rows, rows, rows] + grads + [pl.BlockSpec(up_shape, lambda i: (0, 0))],
        out_shape=[shape_of((n_tok, width))] * 2 + [shape_of((n_tok, width), BF16)] * 2
        + [shape_of(w_out.shape)] * 4 + [shape_of(up_shape)],
        scratch_shapes=[pltpu.VMEM((3 * head_dim, width), BF16), pltpu.VMEM((width, 3 * head_dim), BF16),
                        pltpu.VMEM((width, head_dim), BF16)],
        compiler_params=params(),
        cost_estimate=pl.CostEstimate(flops=24 * n_tok * width * head_dim, bytes_accessed=16 * n_tok * width,
                                      transcendentals=n_tok * group),
        name='attn',
    )(norm_f, dy_one, scales, seq_lens, *w_heads, w_out, dw_up)


def run_widen(x_one, dx_two):
    n_tok, width = x_one.shape
    tile = tile_of(n_tok, 512)
    rows = pl.BlockSpec((tile, width), lambda i: (i, 0))
    return pl.pallas_call(
        widen_kernel,
        grid=(n_tok // tile,),
        in_specs=[rows, rows],
        out_specs=[rows, rows],
        out_shape=[shape_of((n_tok, width))] * 2,
        compiler_params=params(),
        cost_estimate=pl.CostEstimate(flops=n_tok * width, bytes_accessed=12 * n_tok * width, transcendentals=0),
        name='widen',
    )(x_one, dx_two)


def run_exchange(n_dev, call_id, parts, row_arrays, stores, keeps_x2, name):
    side = int(round((n_dev // 2) ** 0.5))
    n_tok, width = parts[0].shape
    n_rows = n_tok // n_dev
    quarter = width // 4

    def blocks(arr):
        return arr.reshape(side, side, 2, n_rows, arr.shape[1]) if arr.shape[0] == n_tok else arr

    sent = [(n_rows, width)] * 2 + ([(16, LANES)] if keeps_x2 else [])
    outs = [shape_of((side, side, 2) + dims, BF16) for dims in sent]
    out_specs = [ANY] * len(outs)
    if keeps_x2:
        outs.append(shape_of((n_rows, width)))
        out_specs.append(pl.BlockSpec(memory_space=pltpu.VMEM))
    kinds = [part.dtype for part in parts]
    scratch = [pltpu.VMEM((4, side, side, n_rows, quarter), kind) for kind in kinds]
    scratch += [pltpu.VMEM((4, side, n_rows, quarter), kind) for kind in kinds]
    scratch += [pltpu.VMEM((4, side - 1, side, n_rows, quarter), kind) for kind in kinds]
    scratch += [pltpu.VMEM((4, side - 1, n_rows, quarter), kind) for kind in kinds]
    scratch += [pltpu.VMEM((n_rows, width), F32)] * 2
    scratch += [pltpu.VMEM(dims, BF16) for dims in sent]
    if keeps_x2:
        scratch.append(pltpu.VMEM((n_rows, LANES), F32))
    scratch += [pltpu.VMEM((n_rows, width), F32)] * len(row_arrays)
    dma = pltpu.SemaphoreType.DMA
    ring, gather_ring = dma((2, 4, side - 1)), dma((3, 4, side - 1))
    scratch += [dma((2, 4, side))] * 2 + [dma((2, 4))] + [ring] * 4 + [dma((len(row_arrays),)), dma((3,))]
    scratch += [gather_ring] * 4 + [dma((3, 4, side))] * 2
    gathered = pl.pallas_call(
        functools.partial(exchange_kernel, side, tuple(row_arrays), stores, keeps_x2),
        in_specs=[ANY] * (2 + len(row_arrays)),
        out_specs=out_specs,
        out_shape=outs,
        scratch_shapes=scratch,
        compiler_params=pltpu.CompilerParams(collective_id=call_id, has_side_effects=True,
                                             vmem_limit_bytes=VMEM_LIMIT),
        name=name,
    )(*map(blocks, parts), *map(blocks, row_arrays.values()))
    return [arr.reshape(-1, arr.shape[-1]) for arr in gathered]


def block_back(carry, seq_lens, layer_w, n_dev):
    w_query, w_key, w_value, w_out, w_up, w_down = layer_w
    act_shape = carry[0].shape
    seq_tok, width = act_shape[1:]
    y_one, y_two, dy_one, dy_two = (a.reshape(-1, width) for a in carry)
    w_heads = [w[:, 0, :].T for w in (w_query, w_key, w_value)]

    g_part, dg_part, dw_up, dw_down = run_ffn(y_one, dy_two, w_up, w_down)
    dy1_b, norm_f, scales, x2_rows = run_exchange(
        n_dev, 0, (dg_part, g_part), {'y_one': y_one, 'y_two': y_two, 'dy_one': dy_one},
        (store_dy1, store_x2), True, 'exchange_g')
    x_two, dy_one, f_part, df_part, *dw_heads, dw_out, dw_up = run_attn(
        seq_tok, norm_f, dy1_b, scales, seq_lens, w_heads, w_out[0], dw_up)
    x1_b, dx2_b = run_exchange(
        n_dev, 1, (f_part, df_part), {'y_one': y_one, 'dy_two': dy_two, 'x_two': x2_rows},
        (store_x1, store_dx2), False, 'exchange_f')
    x_one, dx_two = run_widen(x1_b, dx2_b)
    dw_heads = [dw.T[:, None, :] for dw in dw_heads]
    carry = tuple(a.reshape(act_shape) for a in (x_one, x_two, dy_one, dx_two))
    return carry, (*dw_heads, dw_out[None], dw_up, dw_down)


def stack_grads(grads_by_layer):
    return tuple(jnp.stack([layer_grads[grad_pos] for layer_grads in grads_by_layer]) for grad_pos in range(6))


def solution(mesh):
    act_spec = P('dp', None, None)
    w_specs = (P(None, None, 'tp', None), P(None, None, 'tp', None), P(None, None, 'tp', None),
               P(None, 'tp', None, None), P(None, None, 'tp'), P(None, 'tp', None))
    g_specs = (P('dp', None, 'tp', None), P('dp', None, 'tp', None), P('dp', None, 'tp', None),
               P('dp', 'tp', None, None), P('dp', None, 'tp'), P('dp', 'tp', None))

    def local_fn(y_one, y_two, dy_one, dy_two, seq_lens, w_query, w_key, w_value, w_out, w_up, w_down):
        weights = (w_query, w_key, w_value, w_out, w_up, w_down)
        carry = (y_one, y_two, dy_one, dy_two)
        n_layers, n_dev = w_query.shape[0], mesh.shape['tp']
        grads_by_layer = [None] * n_layers
        for layer_idx in reversed(range(n_layers)):
            layer_w = tuple(w_stack[layer_idx] for w_stack in weights)
            carry, grads_by_layer[layer_idx] = block_back(carry, seq_lens, layer_w, n_dev)
        return carry + stack_grads(grads_by_layer)

    return jax.shard_map(local_fn, mesh=mesh,
                         in_specs=(act_spec,) * 4 + (P('dp'),) + w_specs,
                         out_specs=(act_spec,) * 4 + g_specs,
                         check_vma=False)
```

```python
import functools

import jax
import jax.numpy as jnp
from jax import lax
from jax.experimental import pallas as pl
from jax.experimental.pallas import tpu as pltpu
from jax.sharding import PartitionSpec as P

F32 = jnp.float32
BF16 = jnp.bfloat16
EPS = 1e-5
MASK_VALUE = -1e30
GELU_COEF = 0.044715
GELU_SCALE = (2.0 / jnp.pi) ** 0.5
VMEM_LIMIT = 60 * 1024 * 1024
LANES = 128
MESH = pl.DeviceIdType.MESH
NN = (((1,), (0,)), ((), ()))
NT = (((1,), (1,)), ((), ()))
TN = (((0,), (0,)), ((), ()))


def dot(lhs, rhs, dims=NN):
    return lax.dot_general(lhs, rhs, dims, preferred_element_type=F32)


def rms_norm(x_val):
    inv_rms = lax.rsqrt(jnp.mean(x_val * x_val, axis=-1, keepdims=True) + EPS)
    return x_val * inv_rms, inv_rms


def rms_back(normed, inv_rms, grad_norm):
    return inv_rms * (grad_norm - normed * jnp.mean(grad_norm * normed, axis=-1, keepdims=True))


def gelu_and_slope(x_val):
    tanh_val = jnp.tanh(GELU_SCALE * (x_val + GELU_COEF * (x_val * x_val * x_val)))
    cdf = 0.5 * (1.0 + tanh_val)
    inner_slope = GELU_SCALE * (1.0 + 3.0 * GELU_COEF * (x_val * x_val))
    return x_val * cdf, cdf + x_val * (0.5 * (1.0 - tanh_val * tanh_val) * inner_slope)


def ffn_kernel(y_ref, dy_ref, up_ref, down_ref, branch_ref, dnorm_ref, dup_ref, ddown_ref, up_t, down_t):
    @pl.when(pl.program_id(0) == 0)
    def _():
        up_t[...] = up_ref[...].T
        down_t[...] = down_ref[...].T
        dup_ref[...] = jnp.zeros_like(dup_ref)
        ddown_ref[...] = jnp.zeros_like(ddown_ref)

    norm_b = rms_norm(y_ref[...])[0].astype(BF16)
    dy_b = dy_ref[...].astype(BF16)
    act_val, slope = gelu_and_slope(dot(norm_b, up_ref[...]))
    act_b = act_val.astype(BF16)
    branch_ref[...] = dot(act_b, down_ref[...]).astype(BF16)
    d_pre = (slope * dot(dy_b, down_t[...])).astype(BF16)
    dnorm_ref[...] = dot(d_pre, up_t[...]).astype(BF16)
    ddown_ref[...] += dot(act_b, dy_b, TN)
    dup_ref[...] += dot(d_pre, norm_b, TN)


def attn_kernel(seq_tok, group, n_rows, nf_ref, dy_ref, scale_ref, lens_ref, query_ref, key_ref, value_ref, out_ref, dup_ref,
                x2_ref, dy1_ref, branch_ref, dnorm_ref, dq_ref, dk_ref, dv_ref, dout_ref, dup_t, qkv, qkv_t, out_t):
    head_dim = query_ref.shape[0]
    score_scale = head_dim ** -0.5
    n_tok, width = dy_ref.shape
    grads = (dq_ref, dk_ref, dv_ref)

    @pl.when(pl.program_id(0) == 0)
    def _():
        for k, w_ref in enumerate((query_ref, key_ref, value_ref)):
            qkv[k * head_dim:(k + 1) * head_dim] = w_ref[...]
            grads[k][...] = jnp.zeros_like(grads[k])
        qkv_t[...] = qkv[...].T
        out_t[...] = out_ref[...].T
        dout_ref[...] = jnp.zeros_like(dout_ref)
        dup_t[...] = dup_ref[...].T

    norm_b = nf_ref[...]
    row = lax.broadcasted_iota(jnp.int32, (n_rows, LANES), 0)
    own_lane = lax.broadcasted_iota(jnp.int32, (n_rows, LANES), 1) == row
    for block in range(n_tok // n_rows):
        scales = scale_ref[block * 16:(block + 1) * 16].astype(F32)
        scale = jnp.where(own_lane, scales[:1] + scales[1:2], 0.0)
        at = slice(block * n_rows, (block + 1) * n_rows)
        x2_ref[at] = norm_b[at].astype(F32) * jnp.sum(scale, axis=1, keepdims=True)
    dy_b = dy_ref[...]
    dy1_ref[...] = dy_b.astype(F32)

    proj = dot(norm_b, qkv_t[...]).astype(BF16)
    d_attn = dot(dy_b, out_t[...]).astype(BF16)
    row_pos = lax.broadcasted_iota(jnp.int32, (group, group), 0)
    col_pos = lax.broadcasted_iota(jnp.int32, (group, group), 1)
    causal = (col_pos <= row_pos) & (row_pos // seq_tok == col_pos // seq_tok)
    lane = lax.broadcasted_iota(jnp.int32, (1, group), 1)
    first_seq = pl.program_id(0) * (n_tok // seq_tok)
    attn_parts, dqkv_parts = [], []
    for part in range(n_tok // group):
        rows = slice(part * group, (part + 1) * group)
        query = proj[rows, :head_dim]
        key = proj[rows, head_dim:2 * head_dim]
        value = proj[rows, 2 * head_dim:]
        d_out = d_attn[rows]
        limit = jnp.zeros_like(lane)
        for seq in range(group // seq_tok):
            seq_len = lens_ref[first_seq + part * (group // seq_tok) + seq]
            limit = jnp.where(lane // seq_tok == seq, seq_len, limit)
        visible = causal & (lane % seq_tok < limit)
        scores = jnp.where(visible, dot(query, key, NT) * score_scale, MASK_VALUE)
        expd = jnp.exp(scores - jnp.max(scores, axis=-1, keepdims=True))
        probs = expd / jnp.sum(expd, axis=-1, keepdims=True)
        probs_b = probs.astype(BF16)
        attn_parts.append(dot(probs_b, value).astype(BF16))
        d_value = dot(probs_b, d_out, TN).astype(BF16)
        d_probs = dot(d_out, value, NT)
        row_sum = jnp.sum(d_probs * probs, axis=-1, keepdims=True)
        d_scores = (probs * (d_probs - row_sum) * score_scale).astype(BF16)
        d_query = dot(d_scores, key).astype(BF16)
        d_key = dot(d_scores, query, TN).astype(BF16)
        dqkv_parts.append(jnp.concatenate([d_query, d_key, d_value], axis=1))
    attn = jnp.concatenate(attn_parts, axis=0)
    dqkv = jnp.concatenate(dqkv_parts, axis=0)
    branch_ref[...] = dot(attn, out_ref[...]).astype(BF16)
    dnorm_ref[...] = dot(dqkv, qkv[...]).astype(BF16)
    dout_ref[...] += dot(attn, dy_b, TN)
    d_heads = dot(dqkv, norm_b, TN)
    for k, grad in enumerate(grads):
        grad[...] += d_heads[k * head_dim:(k + 1) * head_dim]


def widen_kernel(x1_in, dx2_in, x1_ref, dx2_ref):
    x1_ref[...] = x1_in[...].astype(F32)
    dx2_ref[...] = dx2_in[...].astype(F32)


def store_x2(total, rows, x2_out, scale_buf, at):
    x_two = rows['y_two'][at] - total[at]
    x2_out[at] = x_two
    normed, inv_rms = rms_norm(x_two)
    scale_buf[at[0]] = jnp.broadcast_to(1.0 / inv_rms, (normed.shape[0], LANES))
    return normed.astype(BF16)


def pack_scales(scale_buf, shape):
    n_rows = scale_buf.shape[0]
    row = lax.broadcasted_iota(jnp.int32, (n_rows, LANES), 0)
    lane = lax.broadcasted_iota(jnp.int32, (n_rows, LANES), 1)
    scale = jnp.sum(jnp.where(row == lane, scale_buf[...], 0.0), axis=0, keepdims=True)
    high = scale.astype(BF16).astype(F32)
    part = lax.broadcasted_iota(jnp.int32, shape, 0)
    return jnp.where(part == 0, high, scale - high).astype(BF16)


def store_dy1(total, rows, x2_out, scale_buf, at):
    return (rows['dy_one'][at] + rms_back(*rms_norm(rows['y_one'][at]), total[at])).astype(BF16)


def store_x1(total, rows, x2_out, scale_buf, at):
    return (rows['y_one'][at] - total[at]).astype(BF16)


def store_dx2(total, rows, x2_out, scale_buf, at):
    return (rows['dy_two'][at] + rms_back(*rms_norm(rows['x_two'][at]), total[at])).astype(BF16)


def exchange_kernel(side, row_names, stores, keeps_x2, *refs):
    n_row = len(row_names)
    parts, row_refs, refs = refs[:2], refs[2:2 + n_row], refs[2 + n_row:]
    n_out = 3 if keeps_x2 else 2
    outs, refs = refs[:n_out], refs[n_out:]
    x2_out = scale_buf = None
    if keeps_x2:
        x2_out, refs = refs[0], refs[1:]
    paired, own, slot_a, slot_b, sums, total, held = (refs[2 * i:2 * i + 2] for i in range(7))
    refs = refs[14:]
    if keeps_x2:
        held, scale_buf, refs = (*held, refs[0]), refs[1], refs[2:]
    row_bufs, refs = dict(zip(row_names, refs[:n_row])), refs[n_row:]
    (pair_send, pair_recv, own_sem, a_send, a_recv, b_send, b_recv, row_sem, out_sem,
     c_send, c_recv, d_send, d_recv, e_send, e_recv) = refs
    steps = side - 1
    n_rows, width = total[0].shape
    quarter = width // 4

    me = lax.axis_index('tp')
    core = me % 2
    pos = {'x': (me // 2) % side, 'y': me // (2 * side)}
    partner = me + 1 - 2 * core
    other = {'x': 'y', 'y': 'x'}
    streams = (('x', 1), ('x', -1), ('y', 1), ('y', -1))

    def wrap(val):
        return (val + 2 * side) % side

    def device(axis, move):
        place = dict(pos)
        place[axis] = wrap(pos[axis] + move)
        return {'tp': (place['y'] * side + place['x']) * 2 + core}

    def cols(k, st):
        return slice(st * quarter, (st + 1) * quarter) if k < 2 else slice(None)

    def lanes(k):
        return range(4 if k < 2 else 1)

    def line(ref, axis, block, *rest):
        return ref.at[(slice(None), block) + rest] if axis == 'x' else ref.at[(block, slice(None)) + rest]

    def remote(src, dst, send, recv, dev):
        return pltpu.make_async_remote_copy(src_ref=src, dst_ref=dst, send_sem=send, recv_sem=recv,
                                            device_id=dev, device_id_type=MESH)

    barrier = pltpu.get_barrier_semaphore()
    neighbours = [{'tp': partner}] + [device(axis, sign) for axis, sign in streams]
    for dev in neighbours:
        pl.semaphore_signal(barrier, inc=1, device_id=dev, device_id_type=MESH)

    row_copies = []
    for i, name in enumerate(row_names):
        src = row_refs[i] if name == 'x_two' else row_refs[i].at[pos['y'], pos['x'], core]
        row_copies.append(pltpu.make_async_copy(src, row_bufs[name], row_sem.at[i]))
        row_copies[-1].start()

    def piece(k, st, turn, whose):
        axis, sign = streams[st]
        return line(parts[k], axis, wrap(pos[axis] - sign * (1 + turn)), whose, slice(None),
                    slice(st * quarter, (st + 1) * quarter))

    def own_copy(k, st, turn):
        return pltpu.make_async_copy(piece(k, st, turn, core), own[k].at[st], own_sem.at[k, st])

    for k in range(2):
        for st in range(4):
            own_copy(k, st, 0).start()
    pl.semaphore_wait(barrier, len(neighbours))

    waits = []
    pair = {}
    for turn in range(side):
        for k in range(2):
            for st in range(4):
                copy = remote(piece(k, st, turn, 1 - core), paired[k].at[st, turn], pair_send.at[k, st, turn],
                              pair_recv.at[k, st, turn], {'tp': partner})
                copy.start()
                pair[k, st, turn] = copy
                waits.append(copy)

    def send_a(k, st, step):
        axis, sign = streams[st]
        if step == 0:
            src = paired[k].at[st, 0]
        else:
            src = slot_a[k].at[st, step - 1]
        copy = remote(src, slot_a[k].at[st, step], a_send.at[k, st, step], a_recv.at[k, st, step], device(axis, sign))
        copy.start()
        waits.append(copy)
        return copy

    def send_b(k, st, step):
        axis, sign = streams[st]
        axis = other[axis]
        if step == 0:
            src = slot_a[k].at[st, steps - 1, wrap(pos[axis] - sign)]
        else:
            src = slot_b[k].at[st, step - 1]
        copy = remote(src, slot_b[k].at[st, step], b_send.at[k, st, step], b_recv.at[k, st, step], device(axis, sign))
        copy.start()
        waits.append(copy)
        return copy

    going = {}
    for turn in range(side):
        for k in range(2):
            for st in range(4):
                if turn:
                    going[k, st].wait_recv()
                pair[k, st, turn].wait_recv()
                own_copy(k, st, turn).wait()

                @pl.loop(0, side)
                def _(j, k=k, st=st, turn=turn):
                    mine = paired[k][st, turn, j].astype(F32) + own[k][st, j].astype(F32)
                    if turn:
                        mine += slot_a[k][st, turn - 1, j].astype(F32)
                        slot_a[k][st, turn - 1, j] = mine.astype(slot_a[k].dtype)
                        if turn == steps:
                            sums[k][st, j] = mine
                    else:
                        paired[k][st, 0, j] = mine.astype(paired[k].dtype)

                if turn < steps:
                    own_copy(k, st, turn + 1).start()
                going[k, st] = send_a(k, st, turn) if turn < steps else send_b(k, st, 0)

    for copy in row_copies:
        copy.wait()

    def gather_b(k, st, step):
        axis, sign = streams[st]
        axis = other[axis]
        block = held[k].at[st, wrap(pos[axis] - sign * step)]
        copy = remote(block, block, c_send.at[k, st, step], c_recv.at[k, st, step], device(axis, sign))
        copy.start()
        waits.append(copy)
        return copy

    def gather_a(k, st, step):
        axis, sign = streams[st]
        group = line(outs[k], axis, wrap(pos[axis] - sign * step), core, slice(None), cols(k, st))
        src = held[k].at[st] if step == 0 else group
        if step < steps:
            copy = remote(src, group, d_send.at[k, st, step], d_recv.at[k, st, step], device(axis, sign))
            copy.start()
            waits.append(copy)
            going[k, st] = copy
        copy = remote(src, group, e_send.at[k, st, step], e_recv.at[k, st, step], {'tp': partner})
        copy.start()
        waits.append(copy)
        last.append(copy)
        if step == 0:
            copy = pltpu.make_async_copy(src, group, out_sem.at[k, st])
            copy.start()
            out_copies.append(copy)

    last, out_copies = [], []
    for step in range(steps):
        for k in range(2):
            for st, (axis, sign) in enumerate(streams):
                going[k, st].wait_recv()
                mine = sums[k].at[st, wrap(pos[other[axis]] - sign * (2 + step))]
                if step + 1 < steps:
                    slot_b[k][st, step] = (slot_b[k][st, step].astype(F32) + mine[...]).astype(slot_b[k].dtype)
                    going[k, st] = send_b(k, st, step + 1)
                else:
                    total[k][:, st * quarter:(st + 1) * quarter] = slot_b[k][st, step].astype(F32) + mine[...]
            if step + 1 == steps:
                @pl.loop(0, n_rows // 16)
                def _(r, k=k):
                    at = (pl.ds(pl.multiple_of(r * 16, 16), 16), slice(0, width))
                    vals = stores[k](total[k], row_bufs, x2_out, scale_buf, at)
                    for st, (axis, sign) in enumerate(streams):
                        held[k][st, pos[other[axis]], at[0]] = vals[:, cols(k, st)]
                ready = [k]
                if k == 1 and n_out == 3:
                    held[2][0, pos['y']] = pack_scales(scale_buf, held[2].shape[2:])
                    ready.append(2)
                for i in ready:
                    for st in lanes(i):
                        going[i, st] = gather_b(i, st, 0)

    for step in range(steps):
        for k in range(n_out):
            for st in lanes(k):
                going[k, st].wait_recv()
                if step + 1 < steps:
                    going[k, st] = gather_b(k, st, step + 1)
                else:
                    gather_a(k, st, 0)
    for step in range(steps):
        for k in range(n_out):
            for st in lanes(k):
                going[k, st].wait_recv()
                gather_a(k, st, step + 1)
    for copy in out_copies:
        copy.wait()
    for copy in last:
        copy.wait_recv()
    for copy in waits:
        copy.wait_send()


def tile_of(n_tok, want):
    tile = want
    while n_tok % tile:
        tile //= 2
    return tile


def shape_of(shape, dtype=F32):
    return jax.ShapeDtypeStruct(shape, dtype)


def params():
    return pltpu.CompilerParams(dimension_semantics=('arbitrary',), vmem_limit_bytes=VMEM_LIMIT)


def whole(arr):
    return pl.BlockSpec(arr.shape, lambda i: (0,) * len(arr.shape))


ANY = pl.BlockSpec(memory_space=pl.ANY)


def run_ffn(y_one, dy_two, w_up, w_down):
    (n_tok, width), cols = y_one.shape, w_up.shape[1]
    tile = tile_of(n_tok, 512)
    rows = pl.BlockSpec((tile, width), lambda i: (i, 0))
    grad = pl.BlockSpec((cols, width), lambda i: (0, 0))
    return pl.pallas_call(
        ffn_kernel,
        grid=(n_tok // tile,),
        in_specs=[rows, rows, whole(w_up), whole(w_down)],
        out_specs=[rows, rows, grad, grad],
        out_shape=[shape_of((n_tok, width), BF16)] * 2 + [shape_of((cols, width))] * 2,
        scratch_shapes=[pltpu.VMEM((cols, width), BF16), pltpu.VMEM((width, cols), BF16)],
        compiler_params=params(),
        cost_estimate=pl.CostEstimate(flops=12 * n_tok * width * cols, bytes_accessed=14 * n_tok * width,
                                      transcendentals=n_tok * cols),
        name='ffn',
    )(y_one, dy_two, w_up, w_down)


def run_attn(seq_tok, norm_f, dy_one, scales, seq_lens, w_heads, w_out, dw_up):
    n_tok, width = dy_one.shape
    head_dim = w_out.shape[0]
    n_rows = n_tok * 16 // scales.shape[0]
    tile = 4 * n_rows
    group = tile_of(tile, 128)
    rows = pl.BlockSpec((tile, width), lambda i: (i, 0))
    grads = [whole(w) for w in w_heads] + [whole(w_out)]
    up_shape = dw_up.shape[::-1]
    return pl.pallas_call(
        functools.partial(attn_kernel, seq_tok, group, n_rows),
        grid=(n_tok // tile,),
        in_specs=[rows, rows, pl.BlockSpec((tile // n_rows * 16, LANES), lambda i: (i, 0)),
                  pl.BlockSpec(memory_space=pltpu.SMEM)] + grads + [whole(dw_up)],
        out_specs=[rows, rows, rows, rows] + grads + [pl.BlockSpec(up_shape, lambda i: (0, 0))],
        out_shape=[shape_of((n_tok, width))] * 2 + [shape_of((n_tok, width), BF16)] * 2
        + [shape_of(w_out.shape)] * 4 + [shape_of(up_shape)],
        scratch_shapes=[pltpu.VMEM((3 * head_dim, width), BF16), pltpu.VMEM((width, 3 * head_dim), BF16),
                        pltpu.VMEM((width, head_dim), BF16)],
        compiler_params=params(),
        cost_estimate=pl.CostEstimate(flops=24 * n_tok * width * head_dim, bytes_accessed=16 * n_tok * width,
                                      transcendentals=n_tok * group),
        name='attn',
    )(norm_f, dy_one, scales, seq_lens, *w_heads, w_out, dw_up)


def run_widen(x_one, dx_two):
    n_tok, width = x_one.shape
    tile = tile_of(n_tok, 768)
    rows = pl.BlockSpec((tile, width), lambda i: (i, 0))
    return pl.pallas_call(
        widen_kernel,
        grid=(n_tok // tile,),
        in_specs=[rows, rows],
        out_specs=[rows, rows],
        out_shape=[shape_of((n_tok, width))] * 2,
        compiler_params=params(),
        cost_estimate=pl.CostEstimate(flops=n_tok * width, bytes_accessed=12 * n_tok * width, transcendentals=0),
        name='widen',
    )(x_one, dx_two)


def run_exchange(n_dev, call_id, parts, row_arrays, stores, keeps_x2, name):
    side = int(round((n_dev // 2) ** 0.5))
    n_tok, width = parts[0].shape
    n_rows = n_tok // n_dev
    quarter = width // 4

    def blocks(arr):
        return arr.reshape(side, side, 2, n_rows, arr.shape[1]) if arr.shape[0] == n_tok else arr

    sent = [(n_rows, width)] * 2 + ([(16, LANES)] if keeps_x2 else [])
    outs = [shape_of((side, side, 2) + dims, BF16) for dims in sent]
    out_specs = [ANY] * len(outs)
    if keeps_x2:
        outs.append(shape_of((n_rows, width)))
        out_specs.append(pl.BlockSpec(memory_space=pltpu.VMEM))
    kinds = [part.dtype for part in parts]
    scratch = [pltpu.VMEM((4, side, side, n_rows, quarter), kind) for kind in kinds]
    scratch += [pltpu.VMEM((4, side, n_rows, quarter), kind) for kind in kinds]
    scratch += [pltpu.VMEM((4, side - 1, side, n_rows, quarter), kind) for kind in kinds]
    scratch += [pltpu.VMEM((4, side - 1, n_rows, quarter), kind) for kind in kinds]
    scratch += [pltpu.VMEM((4, side, n_rows, quarter), F32)] * 2
    scratch += [pltpu.VMEM((n_rows, width), F32)] * 2
    scratch += [pltpu.VMEM((4, side, n_rows, quarter), BF16)] * 2
    if keeps_x2:
        scratch += [pltpu.VMEM((1, side, 16, LANES), BF16), pltpu.VMEM((n_rows, LANES), F32)]
    scratch += [pltpu.VMEM((n_rows, width), F32)] * len(row_arrays)
    dma = pltpu.SemaphoreType.DMA
    ring, gather_ring = dma((2, 4, side - 1)), dma((3, 4, side - 1))
    scratch += [dma((2, 4, side))] * 2 + [dma((2, 4))] + [ring] * 4 + [dma((len(row_arrays),)), dma((3, 4))]
    scratch += [gather_ring] * 4 + [dma((3, 4, side))] * 2
    gathered = pl.pallas_call(
        functools.partial(exchange_kernel, side, tuple(row_arrays), stores, keeps_x2),
        in_specs=[ANY] * (2 + len(row_arrays)),
        out_specs=out_specs,
        out_shape=outs,
        scratch_shapes=scratch,
        compiler_params=pltpu.CompilerParams(collective_id=call_id, has_side_effects=True,
                                             vmem_limit_bytes=VMEM_LIMIT),
        name=name,
    )(*map(blocks, parts), *map(blocks, row_arrays.values()))
    return [arr.reshape(-1, arr.shape[-1]) for arr in gathered]


def block_back(carry, seq_lens, layer_w, n_dev):
    w_query, w_key, w_value, w_out, w_up, w_down = layer_w
    act_shape = carry[0].shape
    seq_tok, width = act_shape[1:]
    y_one, y_two, dy_one, dy_two = (a.reshape(-1, width) for a in carry)
    w_heads = [w[:, 0, :].T for w in (w_query, w_key, w_value)]

    g_part, dg_part, dw_up, dw_down = run_ffn(y_one, dy_two, w_up, w_down)
    dy1_b, norm_f, scales, x2_rows = run_exchange(
        n_dev, 0, (dg_part, g_part), {'y_one': y_one, 'y_two': y_two, 'dy_one': dy_one},
        (store_dy1, store_x2), True, 'exchange_g')
    x_two, dy_one, f_part, df_part, *dw_heads, dw_out, dw_up = run_attn(
        seq_tok, norm_f, dy1_b, scales, seq_lens, w_heads, w_out[0], dw_up)
    x1_b, dx2_b = run_exchange(
        n_dev, 1, (f_part, df_part), {'y_one': y_one, 'dy_two': dy_two, 'x_two': x2_rows},
        (store_x1, store_dx2), False, 'exchange_f')
    x_one, dx_two = run_widen(x1_b, dx2_b)
    dw_heads = [dw.T[:, None, :] for dw in dw_heads]
    carry = tuple(a.reshape(act_shape) for a in (x_one, x_two, dy_one, dx_two))
    return carry, (*dw_heads, dw_out[None], dw_up, dw_down)


def stack_grads(grads_by_layer):
    return tuple(jnp.stack([layer_grads[grad_pos] for layer_grads in grads_by_layer]) for grad_pos in range(6))


def solution(mesh):
    act_spec = P('dp', None, None)
    w_specs = (P(None, None, 'tp', None), P(None, None, 'tp', None), P(None, None, 'tp', None),
               P(None, 'tp', None, None), P(None, None, 'tp'), P(None, 'tp', None))
    g_specs = (P('dp', None, 'tp', None), P('dp', None, 'tp', None), P('dp', None, 'tp', None),
               P('dp', 'tp', None, None), P('dp', None, 'tp'), P('dp', 'tp', None))

    def local_fn(y_one, y_two, dy_one, dy_two, seq_lens, w_query, w_key, w_value, w_out, w_up, w_down):
        weights = (w_query, w_key, w_value, w_out, w_up, w_down)
        carry = (y_one, y_two, dy_one, dy_two)
        n_layers, n_dev = w_query.shape[0], mesh.shape['tp']
        grads_by_layer = [None] * n_layers
        for layer_idx in reversed(range(n_layers)):
            layer_w = tuple(w_stack[layer_idx] for w_stack in weights)
            carry, grads_by_layer[layer_idx] = block_back(carry, seq_lens, layer_w, n_dev)
        return carry + stack_grads(grads_by_layer)

    return jax.shard_map(local_fn, mesh=mesh,
                         in_specs=(act_spec,) * 4 + (P('dp'),) + w_specs,
                         out_specs=(act_spec,) * 4 + g_specs,
                         check_vma=False)
```

```python
import functools

import jax
import jax.numpy as jnp
from jax import lax
from jax.experimental import pallas as pl
from jax.experimental.pallas import tpu as pltpu
from jax.sharding import PartitionSpec as P

F32 = jnp.float32
BF16 = jnp.bfloat16
EPS = 1e-5
MASK_VALUE = -1e30
GELU_COEF = 0.044715
GELU_SCALE = (2.0 / jnp.pi) ** 0.5
VMEM_LIMIT = 60 * 1024 * 1024
LANES = 128
MESH = pl.DeviceIdType.MESH
NN = (((1,), (0,)), ((), ()))
NT = (((1,), (1,)), ((), ()))
TN = (((0,), (0,)), ((), ()))


def dot(lhs, rhs, dims=NN):
    return lax.dot_general(lhs, rhs, dims, preferred_element_type=F32)


def rms_norm(x_val):
    inv_rms = lax.rsqrt(jnp.mean(x_val * x_val, axis=-1, keepdims=True) + EPS)
    return x_val * inv_rms, inv_rms


def rms_back(normed, inv_rms, grad_norm):
    return inv_rms * (grad_norm - normed * jnp.mean(grad_norm * normed, axis=-1, keepdims=True))


def gelu_and_slope(x_val):
    tanh_val = jnp.tanh(GELU_SCALE * (x_val + GELU_COEF * (x_val * x_val * x_val)))
    cdf = 0.5 * (1.0 + tanh_val)
    inner_slope = GELU_SCALE * (1.0 + 3.0 * GELU_COEF * (x_val * x_val))
    return x_val * cdf, cdf + x_val * (0.5 * (1.0 - tanh_val * tanh_val) * inner_slope)


def ffn_kernel(y_ref, dy_ref, up_ref, down_ref, branch_ref, dnorm_ref, dup_ref, ddown_ref, up_t, down_t):
    @pl.when(pl.program_id(0) == 0)
    def _():
        up_t[...] = up_ref[...].T
        down_t[...] = down_ref[...].T
        dup_ref[...] = jnp.zeros_like(dup_ref)
        ddown_ref[...] = jnp.zeros_like(ddown_ref)

    norm_b = rms_norm(y_ref[...])[0].astype(BF16)
    dy_b = dy_ref[...].astype(BF16)
    act_val, slope = gelu_and_slope(dot(norm_b, up_ref[...]))
    act_b = act_val.astype(BF16)
    branch_ref[...] = dot(act_b, down_ref[...]).astype(BF16)
    d_pre = (slope * dot(dy_b, down_t[...])).astype(BF16)
    dnorm_ref[...] = dot(d_pre, up_t[...]).astype(BF16)
    ddown_ref[...] += dot(act_b, dy_b, TN)
    dup_ref[...] += dot(d_pre, norm_b, TN)


def attn_kernel(seq_tok, group, n_rows, nf_ref, dy_ref, scale_ref, lens_ref, query_ref, key_ref, value_ref, out_ref, dup_ref,
                x2_ref, dy1_ref, branch_ref, dnorm_ref, dq_ref, dk_ref, dv_ref, dout_ref, dup_t, qkv, qkv_t, out_t):
    head_dim = query_ref.shape[0]
    score_scale = head_dim ** -0.5
    n_tok, width = dy_ref.shape
    grads = (dq_ref, dk_ref, dv_ref)

    @pl.when(pl.program_id(0) == 0)
    def _():
        for k, w_ref in enumerate((query_ref, key_ref, value_ref)):
            qkv[k * head_dim:(k + 1) * head_dim] = w_ref[...]
            grads[k][...] = jnp.zeros_like(grads[k])
        qkv_t[...] = qkv[...].T
        out_t[...] = out_ref[...].T
        dout_ref[...] = jnp.zeros_like(dout_ref)
        dup_t[...] = dup_ref[...].T

    norm_b = nf_ref[...]
    row = lax.broadcasted_iota(jnp.int32, (n_rows, LANES), 0)
    own_lane = lax.broadcasted_iota(jnp.int32, (n_rows, LANES), 1) == row
    for block in range(n_tok // n_rows):
        scales = scale_ref[block * 16:(block + 1) * 16].astype(F32)
        scale = jnp.where(own_lane, scales[:1] + scales[1:2], 0.0)
        at = slice(block * n_rows, (block + 1) * n_rows)
        x2_ref[at] = norm_b[at].astype(F32) * jnp.sum(scale, axis=1, keepdims=True)
    dy_b = dy_ref[...]
    dy1_ref[...] = dy_b.astype(F32)

    proj = dot(norm_b, qkv_t[...]).astype(BF16)
    d_attn = dot(dy_b, out_t[...]).astype(BF16)
    row_pos = lax.broadcasted_iota(jnp.int32, (group, group), 0)
    col_pos = lax.broadcasted_iota(jnp.int32, (group, group), 1)
    causal = (col_pos <= row_pos) & (row_pos // seq_tok == col_pos // seq_tok)
    lane = lax.broadcasted_iota(jnp.int32, (1, group), 1)
    first_seq = pl.program_id(0) * (n_tok // seq_tok)
    attn_parts, dqkv_parts = [], []
    for part in range(n_tok // group):
        rows = slice(part * group, (part + 1) * group)
        query = proj[rows, :head_dim]
        key = proj[rows, head_dim:2 * head_dim]
        value = proj[rows, 2 * head_dim:]
        d_out = d_attn[rows]
        limit = jnp.zeros_like(lane)
        for seq in range(group // seq_tok):
            seq_len = lens_ref[first_seq + part * (group // seq_tok) + seq]
            limit = jnp.where(lane // seq_tok == seq, seq_len, limit)
        visible = causal & (lane % seq_tok < limit)
        scores = jnp.where(visible, dot(query, key, NT) * score_scale, MASK_VALUE)
        expd = jnp.exp(scores - jnp.max(scores, axis=-1, keepdims=True))
        probs = expd / jnp.sum(expd, axis=-1, keepdims=True)
        probs_b = probs.astype(BF16)
        attn_parts.append(dot(probs_b, value).astype(BF16))
        d_value = dot(probs_b, d_out, TN).astype(BF16)
        d_probs = dot(d_out, value, NT)
        row_sum = jnp.sum(d_probs * probs, axis=-1, keepdims=True)
        d_scores = (probs * (d_probs - row_sum) * score_scale).astype(BF16)
        d_query = dot(d_scores, key).astype(BF16)
        d_key = dot(d_scores, query, TN).astype(BF16)
        dqkv_parts.append(jnp.concatenate([d_query, d_key, d_value], axis=1))
    attn = jnp.concatenate(attn_parts, axis=0)
    dqkv = jnp.concatenate(dqkv_parts, axis=0)
    branch_ref[...] = dot(attn, out_ref[...]).astype(BF16)
    dnorm_ref[...] = dot(dqkv, qkv[...]).astype(BF16)
    dout_ref[...] += dot(attn, dy_b, TN)
    d_heads = dot(dqkv, norm_b, TN)
    for k, grad in enumerate(grads):
        grad[...] += d_heads[k * head_dim:(k + 1) * head_dim]


def widen_kernel(x1_in, dx2_in, x1_ref, dx2_ref):
    x1_ref[...] = x1_in[...].astype(F32)
    dx2_ref[...] = dx2_in[...].astype(F32)


def store_x2(total, rows, x2_out, scale_buf, at):
    x_two = rows['y_two'][at] - total[at]
    x2_out[at] = x_two
    normed, inv_rms = rms_norm(x_two)
    scale_buf[at[0]] = jnp.broadcast_to(1.0 / inv_rms, (normed.shape[0], LANES))
    return normed.astype(BF16)


def pack_scales(scale_buf, shape):
    n_rows = scale_buf.shape[0]
    row = lax.broadcasted_iota(jnp.int32, (n_rows, LANES), 0)
    lane = lax.broadcasted_iota(jnp.int32, (n_rows, LANES), 1)
    scale = jnp.sum(jnp.where(row == lane, scale_buf[...], 0.0), axis=0, keepdims=True)
    high = scale.astype(BF16).astype(F32)
    part = lax.broadcasted_iota(jnp.int32, shape, 0)
    return jnp.where(part == 0, high, scale - high).astype(BF16)


def store_dy1(total, rows, x2_out, scale_buf, at):
    return (rows['dy_one'][at] + rms_back(*rms_norm(rows['y_one'][at]), total[at])).astype(BF16)


def store_x1(total, rows, x2_out, scale_buf, at):
    return (rows['y_one'][at] - total[at]).astype(BF16)


def store_dx2(total, rows, x2_out, scale_buf, at):
    return (rows['dy_two'][at] + rms_back(*rms_norm(rows['x_two'][at]), total[at])).astype(BF16)


def exchange_kernel(side, row_names, stores, keeps_x2, *refs):
    n_row = len(row_names)
    parts, row_refs, refs = refs[:2], refs[2:2 + n_row], refs[2 + n_row:]
    n_out = 3 if keeps_x2 else 2
    outs, refs = refs[:n_out], refs[n_out:]
    x2_out = scale_buf = None
    if keeps_x2:
        x2_out, refs = refs[0], refs[1:]
    paired, own, slot_a, slot_b, sums, held = (refs[4 * i:4 * i + 4] for i in range(6))
    total, refs = refs[24:26], refs[26:]
    if keeps_x2:
        held, scale_buf, refs = (*held, refs[0]), refs[1], refs[2:]
    row_bufs, refs = dict(zip(row_names, refs[:n_row])), refs[n_row:]
    (pair_send, pair_recv, own_sem, a_send, a_recv, b_send, b_recv, row_sem, out_sem,
     c_send, c_recv, d_send, d_recv, e_send, e_recv) = refs
    steps = side - 1
    n_rows, width = total[0].shape
    quarter = width // 8
    units = range(4)
    n_unit = 4 + n_out - 2

    me = lax.axis_index('tp')
    core = me % 2
    pos = {'x': (me // 2) % side, 'y': me // (2 * side)}
    partner = me + 1 - 2 * core
    other = {'x': 'y', 'y': 'x'}
    streams = (('x', 1), ('x', -1), ('y', 1), ('y', -1))

    def wrap(val):
        return (val + 2 * side) % side

    def device(axis, move):
        place = dict(pos)
        place[axis] = wrap(pos[axis] + move)
        return {'tp': (place['y'] * side + place['x']) * 2 + core}

    def cols(k, st):
        start = (k % 2 * 4 + st) * quarter
        return slice(start, start + quarter) if k < 4 else slice(None)

    def lanes(k):
        return range(4 if k < 4 else 1)

    def line(ref, axis, block, *rest):
        return ref.at[(slice(None), block) + rest] if axis == 'x' else ref.at[(block, slice(None)) + rest]

    def remote(src, dst, send, recv, dev):
        return pltpu.make_async_remote_copy(src_ref=src, dst_ref=dst, send_sem=send, recv_sem=recv,
                                            device_id=dev, device_id_type=MESH)

    barrier = pltpu.get_barrier_semaphore()
    neighbours = [{'tp': partner}] + [device(axis, sign) for axis, sign in streams]
    for dev in neighbours:
        pl.semaphore_signal(barrier, inc=1, device_id=dev, device_id_type=MESH)

    row_copies = []
    for i, name in enumerate(row_names):
        src = row_refs[i] if name == 'x_two' else row_refs[i].at[pos['y'], pos['x'], core]
        row_copies.append(pltpu.make_async_copy(src, row_bufs[name], row_sem.at[i]))
        row_copies[-1].start()

    def piece(k, st, turn, whose):
        axis, sign = streams[st]
        return line(parts[k // 2], axis, wrap(pos[axis] - sign * (1 + turn)), whose, slice(None), cols(k, st))

    def own_copy(k, st, turn):
        return pltpu.make_async_copy(piece(k, st, turn, core), own[k].at[st], own_sem.at[k, st])

    for k in units:
        for st in range(4):
            own_copy(k, st, 0).start()
    pl.semaphore_wait(barrier, len(neighbours))

    waits = []
    pair = {}
    for turn in range(side):
        for k in units:
            for st in range(4):
                copy = remote(piece(k, st, turn, 1 - core), paired[k].at[st, turn], pair_send.at[k, st, turn],
                              pair_recv.at[k, st, turn], {'tp': partner})
                copy.start()
                pair[k, st, turn] = copy
                waits.append(copy)

    def send_a(k, st, step):
        axis, sign = streams[st]
        if step == 0:
            src = paired[k].at[st, 0]
        else:
            src = slot_a[k].at[st, step - 1]
        copy = remote(src, slot_a[k].at[st, step], a_send.at[k, st, step], a_recv.at[k, st, step], device(axis, sign))
        copy.start()
        waits.append(copy)
        return copy

    def send_b(k, st, step):
        axis, sign = streams[st]
        axis = other[axis]
        if step == 0:
            src = slot_a[k].at[st, steps - 1, wrap(pos[axis] - sign)]
        else:
            src = slot_b[k].at[st, step - 1]
        copy = remote(src, slot_b[k].at[st, step], b_send.at[k, st, step], b_recv.at[k, st, step], device(axis, sign))
        copy.start()
        waits.append(copy)
        return copy

    going = {}
    for turn in range(side):
        for k in units:
            for st in range(4):
                if turn:
                    going[k, st].wait_recv()
                pair[k, st, turn].wait_recv()
                own_copy(k, st, turn).wait()

                @pl.loop(0, side)
                def _(j, k=k, st=st, turn=turn):
                    mine = paired[k][st, turn, j].astype(F32) + own[k][st, j].astype(F32)
                    if turn:
                        mine += slot_a[k][st, turn - 1, j].astype(F32)
                        slot_a[k][st, turn - 1, j] = mine.astype(slot_a[k].dtype)
                        if turn == steps:
                            sums[k][st, j] = mine
                    else:
                        paired[k][st, 0, j] = mine.astype(paired[k].dtype)

                if turn < steps:
                    own_copy(k, st, turn + 1).start()
                going[k, st] = send_a(k, st, turn) if turn < steps else send_b(k, st, 0)

    for copy in row_copies:
        copy.wait()

    def gather_b(k, st, step):
        axis, sign = streams[st]
        axis = other[axis]
        block = held[k].at[st, wrap(pos[axis] - sign * step)]
        copy = remote(block, block, c_send.at[k, st, step], c_recv.at[k, st, step], device(axis, sign))
        copy.start()
        waits.append(copy)
        return copy

    def gather_a(k, st, step):
        axis, sign = streams[st]
        group = line(outs[k // 2], axis, wrap(pos[axis] - sign * step), core, slice(None), cols(k, st))
        src = held[k].at[st] if step == 0 else group
        if step < steps:
            copy = remote(src, group, d_send.at[k, st, step], d_recv.at[k, st, step], device(axis, sign))
            copy.start()
            waits.append(copy)
            going[k, st] = copy
        copy = remote(src, group, e_send.at[k, st, step], e_recv.at[k, st, step], {'tp': partner})
        copy.start()
        waits.append(copy)
        last.append(copy)
        if step == 0:
            copy = pltpu.make_async_copy(src, group, out_sem.at[k, st])
            copy.start()
            out_copies.append(copy)

    last, out_copies = [], []
    for step in range(steps):
        for k in units:
            for st, (axis, sign) in enumerate(streams):
                going[k, st].wait_recv()
                mine = sums[k].at[st, wrap(pos[other[axis]] - sign * (2 + step))]
                if step + 1 < steps:
                    slot_b[k][st, step] = (slot_b[k][st, step].astype(F32) + mine[...]).astype(slot_b[k].dtype)
                    going[k, st] = send_b(k, st, step + 1)
                else:
                    total[k // 2][:, cols(k, st)] = slot_b[k][st, step].astype(F32) + mine[...]
            if step + 1 == steps and k % 2:
                @pl.loop(0, n_rows // 16)
                def _(r, k=k):
                    at = (pl.ds(pl.multiple_of(r * 16, 16), 16), slice(0, width))
                    vals = stores[k // 2](total[k // 2], row_bufs, x2_out, scale_buf, at)
                    for st, (axis, sign) in enumerate(streams):
                        for unit in (k - 1, k):
                            held[unit][st, pos[other[axis]], at[0]] = vals[:, cols(unit, st)]
                ready = [k - 1, k]
                if k == 3 and n_out == 3:
                    held[4][0, pos['y']] = pack_scales(scale_buf, held[4].shape[2:])
                    ready.append(4)
                for i in ready:
                    for st in lanes(i):
                        going[i, st] = gather_b(i, st, 0)

    for step in range(steps):
        for k in range(n_unit):
            for st in lanes(k):
                going[k, st].wait_recv()
                if step + 1 < steps:
                    going[k, st] = gather_b(k, st, step + 1)
                else:
                    gather_a(k, st, 0)
    for step in range(steps):
        for k in range(n_unit):
            for st in lanes(k):
                going[k, st].wait_recv()
                gather_a(k, st, step + 1)
    for copy in out_copies:
        copy.wait()
    for copy in last:
        copy.wait_recv()
    for copy in waits:
        copy.wait_send()


def tile_of(n_tok, want):
    tile = want
    while n_tok % tile:
        tile //= 2
    return tile


def shape_of(shape, dtype=F32):
    return jax.ShapeDtypeStruct(shape, dtype)


def params():
    return pltpu.CompilerParams(dimension_semantics=('arbitrary',), vmem_limit_bytes=VMEM_LIMIT)


def whole(arr):
    return pl.BlockSpec(arr.shape, lambda i: (0,) * len(arr.shape))


ANY = pl.BlockSpec(memory_space=pl.ANY)


def run_ffn(y_one, dy_two, w_up, w_down):
    (n_tok, width), cols = y_one.shape, w_up.shape[1]
    tile = tile_of(n_tok, 512)
    rows = pl.BlockSpec((tile, width), lambda i: (i, 0))
    grad = pl.BlockSpec((cols, width), lambda i: (0, 0))
    return pl.pallas_call(
        ffn_kernel,
        grid=(n_tok // tile,),
        in_specs=[rows, rows, whole(w_up), whole(w_down)],
        out_specs=[rows, rows, grad, grad],
        out_shape=[shape_of((n_tok, width), BF16)] * 2 + [shape_of((cols, width))] * 2,
        scratch_shapes=[pltpu.VMEM((cols, width), BF16), pltpu.VMEM((width, cols), BF16)],
        compiler_params=params(),
        cost_estimate=pl.CostEstimate(flops=12 * n_tok * width * cols, bytes_accessed=14 * n_tok * width,
                                      transcendentals=n_tok * cols),
        name='ffn',
    )(y_one, dy_two, w_up, w_down)


def run_attn(seq_tok, norm_f, dy_one, scales, seq_lens, w_heads, w_out, dw_up):
    n_tok, width = dy_one.shape
    head_dim = w_out.shape[0]
    n_rows = n_tok * 16 // scales.shape[0]
    tile = 4 * n_rows
    group = tile_of(tile, 128)
    rows = pl.BlockSpec((tile, width), lambda i: (i, 0))
    grads = [whole(w) for w in w_heads] + [whole(w_out)]
    up_shape = dw_up.shape[::-1]
    return pl.pallas_call(
        functools.partial(attn_kernel, seq_tok, group, n_rows),
        grid=(n_tok // tile,),
        in_specs=[rows, rows, pl.BlockSpec((tile // n_rows * 16, LANES), lambda i: (i, 0)),
                  pl.BlockSpec(memory_space=pltpu.SMEM)] + grads + [whole(dw_up)],
        out_specs=[rows, rows, rows, rows] + grads + [pl.BlockSpec(up_shape, lambda i: (0, 0))],
        out_shape=[shape_of((n_tok, width))] * 2 + [shape_of((n_tok, width), BF16)] * 2
        + [shape_of(w_out.shape)] * 4 + [shape_of(up_shape)],
        scratch_shapes=[pltpu.VMEM((3 * head_dim, width), BF16), pltpu.VMEM((width, 3 * head_dim), BF16),
                        pltpu.VMEM((width, head_dim), BF16)],
        compiler_params=params(),
        cost_estimate=pl.CostEstimate(flops=24 * n_tok * width * head_dim, bytes_accessed=16 * n_tok * width,
                                      transcendentals=n_tok * group),
        name='attn',
    )(norm_f, dy_one, scales, seq_lens, *w_heads, w_out, dw_up)


def run_widen(x_one, dx_two):
    n_tok, width = x_one.shape
    tile = tile_of(n_tok, 768)
    rows = pl.BlockSpec((tile, width), lambda i: (i, 0))
    return pl.pallas_call(
        widen_kernel,
        grid=(n_tok // tile,),
        in_specs=[rows, rows],
        out_specs=[rows, rows],
        out_shape=[shape_of((n_tok, width))] * 2,
        compiler_params=params(),
        cost_estimate=pl.CostEstimate(flops=n_tok * width, bytes_accessed=12 * n_tok * width, transcendentals=0),
        name='widen',
    )(x_one, dx_two)


def run_exchange(n_dev, call_id, parts, row_arrays, stores, keeps_x2, name):
    side = int(round((n_dev // 2) ** 0.5))
    n_tok, width = parts[0].shape
    n_rows = n_tok // n_dev
    quarter = width // 8

    def blocks(arr):
        return arr.reshape(side, side, 2, n_rows, arr.shape[1]) if arr.shape[0] == n_tok else arr

    sent = [(n_rows, width)] * 2 + ([(16, LANES)] if keeps_x2 else [])
    outs = [shape_of((side, side, 2) + dims, BF16) for dims in sent]
    out_specs = [ANY] * len(outs)
    if keeps_x2:
        outs.append(shape_of((n_rows, width)))
        out_specs.append(pl.BlockSpec(memory_space=pltpu.VMEM))
    turns = (4, side, n_rows, quarter)
    scratch = [pltpu.VMEM((4, side) + turns[1:], BF16)] * 4 + [pltpu.VMEM(turns, BF16)] * 4
    scratch += [pltpu.VMEM((4, side - 1) + turns[1:], BF16)] * 4
    scratch += [pltpu.VMEM((4, side - 1, n_rows, quarter), BF16)] * 4
    scratch += [pltpu.VMEM(turns, F32)] * 4 + [pltpu.VMEM(turns, BF16)] * 4
    scratch += [pltpu.VMEM((n_rows, width), F32)] * 2
    if keeps_x2:
        scratch += [pltpu.VMEM((1, side, 16, LANES), BF16), pltpu.VMEM((n_rows, LANES), F32)]
    scratch += [pltpu.VMEM((n_rows, width), F32)] * len(row_arrays)
    dma = pltpu.SemaphoreType.DMA
    ring, gather_ring = dma((4, 4, side - 1)), dma((5, 4, side - 1))
    scratch += [dma((4, 4, side))] * 2 + [dma((4, 4))] + [ring] * 4 + [dma((len(row_arrays),)), dma((5, 4))]
    scratch += [gather_ring] * 4 + [dma((5, 4, side))] * 2
    gathered = pl.pallas_call(
        functools.partial(exchange_kernel, side, tuple(row_arrays), stores, keeps_x2),
        in_specs=[ANY] * (2 + len(row_arrays)),
        out_specs=out_specs,
        out_shape=outs,
        scratch_shapes=scratch,
        compiler_params=pltpu.CompilerParams(collective_id=call_id, has_side_effects=True,
                                             vmem_limit_bytes=VMEM_LIMIT),
        name=name,
    )(*map(blocks, parts), *map(blocks, row_arrays.values()))
    return [arr.reshape(-1, arr.shape[-1]) for arr in gathered]


def block_back(carry, seq_lens, layer_w, n_dev):
    w_query, w_key, w_value, w_out, w_up, w_down = layer_w
    act_shape = carry[0].shape
    seq_tok, width = act_shape[1:]
    y_one, y_two, dy_one, dy_two = (a.reshape(-1, width) for a in carry)
    w_heads = [w[:, 0, :].T for w in (w_query, w_key, w_value)]

    g_part, dg_part, dw_up, dw_down = run_ffn(y_one, dy_two, w_up, w_down)
    dy1_b, norm_f, scales, x2_rows = run_exchange(
        n_dev, 0, (dg_part, g_part), {'y_one': y_one, 'y_two': y_two, 'dy_one': dy_one},
        (store_dy1, store_x2), True, 'exchange_g')
    x_two, dy_one, f_part, df_part, *dw_heads, dw_out, dw_up = run_attn(
        seq_tok, norm_f, dy1_b, scales, seq_lens, w_heads, w_out[0], dw_up)
    x1_b, dx2_b = run_exchange(
        n_dev, 1, (f_part, df_part), {'y_one': y_one, 'dy_two': dy_two, 'x_two': x2_rows},
        (store_x1, store_dx2), False, 'exchange_f')
    x_one, dx_two = run_widen(x1_b, dx2_b)
    dw_heads = [dw.T[:, None, :] for dw in dw_heads]
    carry = tuple(a.reshape(act_shape) for a in (x_one, x_two, dy_one, dx_two))
    return carry, (*dw_heads, dw_out[None], dw_up, dw_down)


def stack_grads(grads_by_layer):
    return tuple(jnp.stack([layer_grads[grad_pos] for layer_grads in grads_by_layer]) for grad_pos in range(6))


def solution(mesh):
    act_spec = P('dp', None, None)
    w_specs = (P(None, None, 'tp', None), P(None, None, 'tp', None), P(None, None, 'tp', None),
               P(None, 'tp', None, None), P(None, None, 'tp'), P(None, 'tp', None))
    g_specs = (P('dp', None, 'tp', None), P('dp', None, 'tp', None), P('dp', None, 'tp', None),
               P('dp', 'tp', None, None), P('dp', None, 'tp'), P('dp', 'tp', None))

    def local_fn(y_one, y_two, dy_one, dy_two, seq_lens, w_query, w_key, w_value, w_out, w_up, w_down):
        weights = (w_query, w_key, w_value, w_out, w_up, w_down)
        carry = (y_one, y_two, dy_one, dy_two)
        n_layers, n_dev = w_query.shape[0], mesh.shape['tp']
        grads_by_layer = [None] * n_layers
        for layer_idx in reversed(range(n_layers)):
            layer_w = tuple(w_stack[layer_idx] for w_stack in weights)
            carry, grads_by_layer[layer_idx] = block_back(carry, seq_lens, layer_w, n_dev)
        return carry + stack_grads(grads_by_layer)

    return jax.shard_map(local_fn, mesh=mesh,
                         in_specs=(act_spec,) * 4 + (P('dp'),) + w_specs,
                         out_specs=(act_spec,) * 4 + g_specs,
                         check_vma=False)
```
